128 devices in a mesh: comp: 4 (over x), tile: 32 (over y, z, core).
Axes of the slice: x: 4, y: 4, z: 4, core: 2. Of those that a mesh axis runs over, the one named last changes fastest.
Arguments:
- atmos_column_state: float32 [128, 524288], P(None, ('comp', 'tile')), may hold values from -6 to 6
- vertical_column_operator: float32 [128, 128], replicated, may hold values from -0.5 to 0.5
- level_flux_weight: float32 [128], replicated, may hold values from -0.5 to 0.5
- coupling_response: float32 [128], replicated, may hold values from -4 to 4
- remap_weight_blocks: bfloat16 [8, 128, 128], replicated, may hold values from -0.5 to 0.5
- remap_source_row: int32 [40960, 4], P('tile'), may hold values from 0 to 4095
- remap_entry_block: int32 [40960, 4], P('tile'), may hold values from 0 to 7
- remap_entry_present: int32 [40960, 4], P('tile'), may hold values from 0 to 1, as said below
- ocean_land_mask: int32 [2048, 2560], P('tile'), may hold values 0 or 1
- depth_diagonal_added: float32 [2048, 2560], P('tile'), may hold values from 0.001 to 0.1
- ocean_surface_temp: float32 [2048, 2560], P('tile'), may hold values from -6 to 6
- sea_temp_source_row: int32 [4096], P(('comp', 'tile')), may hold values from 0 to 40959
Outputs:
- atm_out: float32 [128, 524288], P(None, ('comp', 'tile'))
- surface_height: float32 [2048, 2560], P('tile')
The draws below stay inside these ranges and needn't reach their ends.
Inputs may be any that keep to these rules, and one draw needn't show every extreme that they name: `remap_entry_present`: 1 where the entry counts, 0 where it doesn't.
All inputs are finite; a program needn't handle non-finite values. No bound on the sum of `ocean_land_mask` on one device may be relied on, other than what follows from the above.
Results may differ from the reference program's by a relative error of at most 0.0029.
Values may be sent and summed in bfloat16 or wider, within the bound.
A program may use at most 64 MiB of HBM per device.

```python
import math
import jax
import jax.numpy as jnp
from jax import lax

LEV = 128
ROW_POINTS = 128
NW = 8
K = 4
ITERS = 3
SUBSTEPS = 2
OX_DEV = 64
OY = 2560
COLS = 524288
ATMOS_FLUX_ROWS = 4096
NOX = 2048
OCEAN_FLUX_ROWS = 40960


def remap_table(key):
    per_grid = OY // ROW_POINTS
    block_grid = 4 * OX_DEV
    source = jax.random.randint(jax.random.fold_in(key, 101), (OCEAN_FLUX_ROWS, K), 0, ATMOS_FLUX_ROWS, dtype=jnp.int32)
    blocks = jax.random.randint(jax.random.fold_in(key, 102), (OCEAN_FLUX_ROWS, K), 0, NW, dtype=jnp.int32)
    present = (jax.random.randint(jax.random.fold_in(key, 103), (OCEAN_FLUX_ROWS, K), 0, 4, dtype=jnp.int32) < 3).astype(jnp.int32)
    parity = jax.random.randint(jax.random.fold_in(key, 104), (), 0, 2, dtype=jnp.int32)
    flux_index = jnp.arange(OCEAN_FLUX_ROWS, dtype=jnp.int32)
    grid_row = flux_index // per_grid
    within = flux_index % per_grid
    region = grid_row // block_grid
    smooth = (region + parity) % 2 == 0
    base_row = (region * block_grid * per_grid + within).astype(jnp.int32)
    common = jnp.arange(K, dtype=jnp.int32) < K - 1
    shared = jnp.logical_and(smooth[:, None], common[None, :])
    source = jnp.where(shared, source[base_row], source)
    blocks = jnp.where(shared, blocks[base_row], blocks)
    present = jnp.where(shared, jnp.ones_like(present), present)
    return (source, blocks, present)


def draw_remap_source_row(key, part):
    return remap_table(key)[0]


def draw_remap_entry_block(key, part):
    return remap_table(key)[1]


def draw_remap_entry_present(key, part):
    return remap_table(key)[2]


def with_ends(array, own_key, low, top_value):
    index_at = [jax.random.randint(jax.random.fold_in(own_key, axis), (), 0, length) for axis, length in enumerate(array.shape)]
    widest = array.shape.index(max(array.shape))
    next_to = index_at[:widest] + [(index_at[widest] + 1) % array.shape[widest]] + index_at[widest + 1:]
    return array.at[tuple(index_at)].set(low).at[tuple(next_to)].set(top_value)


def block_scale(key, extent, pieces, smallest, top_value):
    loudness = 1.0
    for position, blocks in pieces:
        heights = jax.random.uniform(jax.random.fold_in(jax.random.fold_in(key, 6), position), (blocks,), jnp.float32, smallest / len(pieces), top_value / len(pieces))
        loudness = loudness * jnp.repeat(jnp.exp(heights), extent[position] // blocks).reshape((-1,) + (1,) * (len(extent) - 1 - position))
    return loudness


def bell_draw(own_key, extent, width, most, split=(), kind=jnp.bfloat16):
    drawn = jax.random.normal(own_key, extent, jnp.float32) * width
    if len(split) > 0:
        drawn = block_scale(own_key, extent, split, -0.22, 0.18) * drawn
    return jnp.clip(drawn, min=-most, max=most).astype(kind)


def setup_inputs(seed: int = 0) -> dict:
    seeds = jax.random.split(jax.random.key(seed), 13)
    return {
        "atmos_column_state": bell_draw(seeds[0], (LEV, COLS), 1.0, 6.0, ((1, 128),), jnp.float32),
        "vertical_column_operator": bell_draw(seeds[1], (LEV, LEV), LEV ** -0.5, 0.5, (), jnp.float32),
        "level_flux_weight": bell_draw(seeds[2], (LEV,), LEV ** -0.5, 0.5, (), jnp.float32),
        "coupling_response": bell_draw(seeds[3], (LEV,), 1.0, 4.0, (), jnp.float32),
        "remap_weight_blocks": bell_draw(seeds[4], (NW, ROW_POINTS, ROW_POINTS), ROW_POINTS ** -0.5, 0.5),
        "remap_source_row": draw_remap_source_row(jax.random.fold_in(seeds[12], 71), 0),
        "remap_entry_block": draw_remap_entry_block(jax.random.fold_in(seeds[12], 71), 0),
        "remap_entry_present": draw_remap_entry_present(jax.random.fold_in(seeds[12], 71), 0),
        "ocean_land_mask": with_ends((jax.random.randint(seeds[8], (NOX, OY), 0, 10) < 7).astype(jnp.int32), jax.random.fold_in(seeds[8], 1), 0, 1),
        "depth_diagonal_added": jnp.clip(jnp.exp(math.log(0.1) - 4.6051702 * jax.random.uniform(seeds[9], (NOX, OY), jnp.float32) ** block_scale(seeds[9], (NOX, OY), ((0, 32),), -0.2, 0.2)), 0.001, 0.1),
        "ocean_surface_temp": bell_draw(seeds[10], (NOX, OY), 1.0, 6.0, ((0, 32),), jnp.float32),
        "sea_temp_source_row": with_ends(jax.random.randint(seeds[11], (ATMOS_FLUX_ROWS,), 0, OCEAN_FLUX_ROWS), jax.random.fold_in(seeds[11], 1), 0, OCEAN_FLUX_ROWS - 1).astype(jnp.int32),
    }


time_step = 0.5


def advance(state, vertical_column_operator):
    return state + time_step * jnp.tanh(jnp.dot(vertical_column_operator, state, precision=lax.Precision.HIGHEST, preferred_element_type=jnp.float32))


def apply_table(chosen, remap_entry_block, remap_entry_present, remap_weight_blocks):
    blocks = remap_entry_block.reshape(-1)
    live = remap_entry_present.reshape(-1)
    total = jnp.zeros((chosen.shape[0], remap_weight_blocks.shape[2]), jnp.float32)
    for which in range(remap_weight_blocks.shape[0]):
        keep = jnp.logical_and(blocks == which, live == 1)
        masked = jnp.where(keep[:, None], chosen, jnp.zeros_like(chosen))
        total = total + jnp.dot(masked, remap_weight_blocks[which], preferred_element_type=jnp.float32)
    return total.reshape(remap_entry_block.shape[0], remap_entry_block.shape[1], -1).sum(axis=1)


def operate(field, mask_floating, depth_diagonal_added):
    masked = mask_floating * field
    padded = jnp.pad(masked, ((1, 1), (0, 0)))
    beside = padded[2:] + padded[:-2] + jnp.roll(masked, 1, axis=1) + jnp.roll(masked, -1, axis=1)
    return mask_floating * ((4.0 + depth_diagonal_added) * field - beside) + (1.0 - mask_floating) * field


def reference(atmos_column_state, vertical_column_operator, level_flux_weight, coupling_response, remap_weight_blocks, remap_source_row, remap_entry_block, remap_entry_present, ocean_land_mask, depth_diagonal_added, ocean_surface_temp, sea_temp_source_row):
    state = atmos_column_state
    for substep in range(SUBSTEPS):
        state = advance(state, vertical_column_operator)
    flux = jnp.dot(level_flux_weight, state, precision=lax.Precision.HIGHEST, preferred_element_type=jnp.float32)
    flux_rows = flux.reshape(-1, ROW_POINTS).astype(jnp.bfloat16)
    chosen = flux_rows[remap_source_row.reshape(-1)]
    forcing = apply_table(chosen, remap_entry_block, remap_entry_present, remap_weight_blocks).reshape(NOX, OY)
    mask_floating = ocean_land_mask.astype(jnp.float32)
    rhs = mask_floating * forcing
    diag = mask_floating * (4.0 + depth_diagonal_added) + (1.0 - mask_floating)
    solved_field = jnp.zeros_like(rhs)
    residual = rhs
    precond = residual / diag
    direction = precond
    rz_now = jnp.sum(residual * precond)
    for step in range(ITERS):
        image = operate(direction, mask_floating, depth_diagonal_added)
        alpha = rz_now / jnp.sum(direction * image)
        solved_field = solved_field + alpha * direction
        residual = residual - alpha * image
        precond = residual / diag
        rz_next = jnp.sum(residual * precond)
        direction = precond + (rz_next / rz_now) * direction
        rz_now = rz_next
    sea_surface_temp = (mask_floating * (ocean_surface_temp + solved_field)).astype(jnp.bfloat16).reshape(-1, ROW_POINTS)
    received_rows = sea_surface_temp[sea_temp_source_row].astype(jnp.float32).reshape(-1)
    tend = jnp.tanh(jnp.dot(vertical_column_operator, state, precision=lax.Precision.HIGHEST, preferred_element_type=jnp.float32))
    atm_out = state + time_step * (tend + coupling_response[:, None] * received_rows[None, :])
    return atm_out, solved_field
```

```python
import functools

import jax
import jax.numpy as jnp
from jax import lax
from jax.experimental import pallas as pl
from jax.experimental.pallas import tpu as pltpu
from jax.sharding import PartitionSpec as P

F32, BF16, I32 = jnp.float32, jnp.bfloat16, jnp.int32
MESH = pl.DeviceIdType.MESH
LANES = 128
HALO = 8
TIME_STEP = 0.5


def kernel(
    groups,
    tiles,
    state_hbm,
    vco_ref,
    weight_ref,
    blocks_ref,
    source_ref,
    entry_ref,
    present_ref,
    mask_ref,
    depth_ref,
    temp_ref,
    wanted_ref,
    pre_hbm,
    height_hbm,
    rows_out,
    state,
    vv,
    fluxf,
    flux_all,
    table,
    idx_v,
    idx_s,
    coef,
    field,
    w0,
    w1,
    w2,
    height,
    req_v,
    picks,
    sst,
    rows_send,
    rows_recv,
    gram_send,
    gram_recv,
    in_sem,
    out_sem,
    idx_sem,
    height_sem,
    flux_ssem,
    flux_rsem,
    req_ssem,
    req_rsem,
    halo_ssem,
    halo_rsem,
    gram_ssem,
    gram_rsem,
    rows_ssem,
    rows_rsem,
):
    group, tile = lax.axis_index("comp"), lax.axis_index("tile")
    count = groups * tiles
    me = group * tiles + tile
    lev, cols = state.shape
    own = mask_ref.shape[0]
    width = mask_ref.shape[1]
    per = width // LANES
    ext = own + 2 * HALO
    nrows = cols // LANES
    n_flux = count * nrows
    n_ocean = source_ref.shape[1]
    n_block = blocks_ref.shape[0]
    chunk = min(1024, cols)
    n_chunk = cols // chunk

    def peer_of(i):
        other = lax.rem(me + i, count)
        return lax.div(other, tiles), lax.rem(other, tiles), other

    barrier = pltpu.get_barrier_semaphore()

    def greet(i, carry):
        g, t, _ = peer_of(i)
        pl.semaphore_signal(barrier, inc=1, device_id=(g, t), device_id_type=MESH)
        return carry

    lax.fori_loop(1, count, greet, 0)

    def load_state(i):
        part = pl.ds(i * chunk, chunk)
        return pltpu.make_async_copy(state_hbm.at[:, part], state.at[:, part], in_sem.at[i])

    for i in range(n_chunk):
        load_state(i).start()

    vco = vco_ref[...]
    v_hi = vco.astype(BF16)
    v_lo = (vco - v_hi.astype(F32)).astype(BF16)
    vv[0:lev, 0:lev] = v_hi
    vv[0:lev, lev : 2 * lev] = v_hi
    vv[lev : 2 * lev, 0:lev] = v_lo
    vv[lev : 2 * lev, lev : 2 * lev] = v_lo

    mask = mask_ref[...].astype(F32)
    coef[HALO : HALO + own, :] = mask * (4.0 + depth_ref[...])
    spare = n_block * n_flux
    index = jnp.where(
        present_ref[...] == 1, entry_ref[...] * n_flux + source_ref[...], jnp.full(source_ref.shape, spare, I32)
    )
    idx_v[:, LANES : LANES + n_ocean] = index
    req_v[pl.ds(tile * 8, 8), :] = wanted_ref[...]
    table[pl.ds(spare, 8), :] = jnp.zeros((8, LANES), F32)

    def tendency(s):
        hi = s.astype(BF16)
        lo = (s - hi.astype(F32)).astype(BF16)
        both = jnp.dot(vv[...], jnp.concatenate([hi, lo], axis=0), preferred_element_type=F32)
        return TIME_STEP * jnp.tanh(both[0:lev] + both[lev : 2 * lev])

    column = weight_ref[...]

    def first_steps(i):
        load_state(i).wait()
        part = pl.ds(i * chunk, chunk)
        s = state[:, part]
        s = s + tendency(s)
        s = s + tendency(s)
        state[:, part] = s
        line = jnp.sum(s * column, axis=0, keepdims=True)
        for k in range(chunk // LANES):
            fluxf[i * (chunk // LANES) + k : i * (chunk // LANES) + k + 1, :] = line[:, k * LANES : (k + 1) * LANES]

    for i in range(n_chunk - 1):
        first_steps(i)
    pl.semaphore_wait(barrier, count - 1)

    after, before = lax.rem(tile + 1, tiles), lax.rem(tile + tiles - 1, tiles)

    def halo(ref, src, dst, k, target):
        return pltpu.make_async_remote_copy(
            src_ref=ref.at[src],
            dst_ref=ref.at[dst],
            send_sem=halo_ssem.at[k],
            recv_sem=halo_rsem.at[k],
            device_id=(group, target),
            device_id_type=MESH,
        )

    everything = slice(None)
    halos = (
        halo(coef, (pl.ds(own, HALO), everything), (pl.ds(0, HALO), everything), 0, after),
        halo(coef, (pl.ds(HALO, HALO), everything), (pl.ds(HALO + own, HALO), everything), 1, before),
        halo(idx_v, (everything, pl.ds(n_ocean, LANES)), (everything, pl.ds(0, LANES)), 2, after),
        halo(idx_v, (everything, pl.ds(LANES, LANES)), (everything, pl.ds(LANES + n_ocean, LANES)), 3, before),
    )
    for copy in halos:
        copy.start()

    def request(i):
        other = lax.rem(tile + i, tiles)
        slot = pl.ds(tile * 8, 8)
        return pltpu.make_async_remote_copy(
            src_ref=req_v.at[slot],
            dst_ref=req_v.at[slot],
            send_sem=req_ssem.at[i],
            recv_sem=req_rsem.at[i],
            device_id=(group, other),
            device_id_type=MESH,
        )

    def each(make, what, first, last):
        def step(i, carry):
            what(make(i))
            return carry

        lax.fori_loop(first, last, step, 0)

    start, sent, arrived = (lambda c: c.start()), (lambda c: c.wait_send()), (lambda c: c.wait_recv())
    each(request, start, 1, tiles)

    first_steps(n_chunk - 1)
    mine = pl.ds(pl.multiple_of(me * nrows, nrows), nrows)
    flux_all[mine, :] = fluxf[...].astype(BF16)

    def flux_copy(i):
        g, t, _ = peer_of(i)
        return pltpu.make_async_remote_copy(
            src_ref=flux_all.at[mine],
            dst_ref=flux_all.at[mine],
            send_sem=flux_ssem.at[i],
            recv_sem=flux_rsem.at[i],
            device_id=(g, t),
            device_id_type=MESH,
        )

    each(flux_copy, start, 1, count)

    def store_pre(i):
        part = pl.ds(i * chunk, chunk)
        return pltpu.make_async_copy(state.at[:, part], pre_hbm.at[:, part], out_sem.at[i])

    for i in range(n_chunk):
        part = pl.ds(i * chunk, chunk)
        s = state[:, part]
        state[:, part] = s + tendency(s)
        store_pre(i).start()

    for copy in halos:
        copy.wait()
    index_copy = pltpu.make_async_copy(idx_v, idx_s, idx_sem)
    index_copy.start()
    each(request, arrived, 1, tiles)

    base = tile * n_ocean
    where_col = lax.broadcasted_iota(I32, (nrows, n_ocean), 1)
    stacked = (lax.rem(where_col, own)) * per + lax.div(where_col, own)

    def pick(t, carry):
        block = req_v[pl.ds(pl.multiple_of(t * 8, 8), 8), :]
        col = jnp.transpose(jnp.broadcast_to(block[0:1, :], (LANES, LANES)))[0:nrows, 0:1] - base
        hit = jnp.where(col == stacked, 1.0, 0.0).astype(BF16)
        picks[pl.ds(pl.multiple_of(t * nrows, nrows), nrows), :] = hit
        return carry

    lax.fori_loop(0, tiles, pick, 0)

    inner = jnp.where(coef[...] > 0.0, 1.0 / coef[...], 0.0)
    coef[...] = inner
    coef[0:HALO, :] = jnp.where(tile > 0, inner[0:HALO], 0.0)
    coef[HALO + own : ext, :] = jnp.where(tile < tiles - 1, inner[HALO + own : ext], 0.0)

    each(flux_copy, arrived, 1, count)
    rows_at_once = min(512, n_flux)

    def products(i, carry):
        at = pl.multiple_of(i * rows_at_once, rows_at_once)
        some = flux_all[pl.ds(at, rows_at_once), :]
        for b in range(0, n_block, 2):
            pair = jnp.concatenate([blocks_ref[b], blocks_ref[b + 1]], axis=1)
            got = jnp.dot(some, pair, preferred_element_type=F32)
            table[pl.ds(pl.multiple_of(b * n_flux + at, rows_at_once), rows_at_once), :] = got[:, 0:LANES]
            table[pl.ds(pl.multiple_of((b + 1) * n_flux + at, rows_at_once), rows_at_once), :] = got[:, LANES:]
        return carry

    lax.fori_loop(0, n_flux // rows_at_once, products, 0)

    index_copy.wait()
    zero_rows = jnp.zeros((HALO, width), F32)
    field[0:HALO, :] = zero_rows
    field[HALO + own : ext, :] = zero_rows

    def forcing_row(g_tile, s, j):
        e = (g_tile * 8 + s - HALO) * per + j + LANES
        total = table[pl.ds(idx_s[0, e], 1), :]
        for k in range(1, 4):
            total = total + table[pl.ds(idx_s[k, e], 1), :]
        at = pl.multiple_of(g_tile * 8, 8)
        block = field.at[pl.ds(at, 8), pl.ds(pl.multiple_of(j * LANES, LANES), LANES)]
        block[s : s + 1, :] = total

    def edge(j, carry):
        for s in (HALO - 3, HALO - 2, HALO - 1):
            forcing_row(0, s, j)
        for s in (0, 1, 2):
            forcing_row(ext // 8 - 1, s, j)
        return carry

    lax.fori_loop(0, per, edge, 0)

    def inside_rows(n, carry):
        g_tile, j = 1 + lax.div(n, per), lax.rem(n, per)
        for s in range(8):
            forcing_row(g_tile, s, j)
        return carry

    lax.fori_loop(0, own // 8 * per, inside_rows, 0)

    n_tile = ext // 8
    top = lax.broadcasted_iota(I32, (8, width), 0) == 0
    bottom = lax.broadcasted_iota(I32, (8, width), 0) == 7

    def rows8(ref, k):
        return ref[pl.ds(pl.multiple_of(k * 8, 8), 8), :]

    def beside(ref, k):
        here = rows8(ref, k)
        above = rows8(ref, jnp.maximum(k - 1, 0))
        below = rows8(ref, jnp.minimum(k + 1, n_tile - 1))
        up = jnp.where(top, pltpu.roll(above, 1, 0), pltpu.roll(here, 1, 0))
        down = jnp.where(bottom, pltpu.roll(below, 7, 0), pltpu.roll(here, 7, 0))
        return up + down + pltpu.roll(here, 1, 1) + pltpu.roll(here, width - 1, 1)

    def folded(value):
        total = value[:, 0:LANES]
        for k in range(1, per):
            total = total + value[:, k * LANES : (k + 1) * LANES]
        return total

    nothing = jnp.zeros((8, LANES), F32)

    def first(k, carry):
        f = rows8(field, k)
        w = rows8(coef, k) * f
        w0[pl.ds(pl.multiple_of(k * 8, 8), 8), :] = w
        inside = jnp.logical_and(k >= 1, k < n_tile - 1)
        return carry + jnp.where(inside, folded(w * f), 0.0)

    nu0 = lax.fori_loop(0, n_tile, first, nothing)

    def apply(w_old, w_new, k, carry):
        a, b = carry
        q = rows8(field, k) - beside(w_old, k)
        w = rows8(coef, k) * q
        field[pl.ds(pl.multiple_of(k * 8, 8), 8), :] = q
        w_new[pl.ds(pl.multiple_of(k * 8, 8), 8), :] = w
        inside = jnp.logical_and(k >= 1, k < n_tile - 1)
        a = a + jnp.where(inside, folded(rows8(w_old, k) * q), 0.0)
        b = b + jnp.where(inside, folded(w * q), 0.0)
        return a, b

    nu1, nu2 = lax.fori_loop(0, n_tile, functools.partial(apply, w0, w1), (nothing, nothing))
    nu3, nu4 = lax.fori_loop(0, n_tile, functools.partial(apply, w1, w2), (nothing, nothing))

    def last(k, carry):
        q = rows8(field, k) - beside(w2, k)
        return carry + folded(rows8(w2, k) * q)

    nu5 = lax.fori_loop(1, n_tile - 1, last, nothing)

    gram_send[...] = jnp.zeros((8, LANES), F32)
    for k, nu in enumerate((nu0, nu1, nu2, nu3, nu4, nu5)):
        gram_send[k : k + 1, :] = jnp.sum(nu, axis=0, keepdims=True)
    gram_slot = pl.ds(pl.multiple_of(tile * 8, 8), 8)
    gram_recv[gram_slot, :] = gram_send[...]

    def gram_copy(i):
        return pltpu.make_async_remote_copy(
            src_ref=gram_send,
            dst_ref=gram_recv.at[gram_slot],
            send_sem=gram_ssem.at[i],
            recv_sem=gram_rsem.at[i],
            device_id=(group, lax.rem(tile + i, tiles)),
            device_id_type=MESH,
        )

    each(gram_copy, start, 1, tiles)
    each(gram_copy, arrived, 1, tiles)
    total = jnp.sum(gram_recv[...].reshape(tiles, 8, LANES), axis=0)
    total = jnp.sum(total, axis=1, keepdims=True)
    n0, n1, n2, n3, n4, n5 = (total[k : k + 1, :] for k in range(6))

    def inverse(pivot, scale):
        good = pivot > 1e-6 * scale
        return jnp.where(good, 1.0 / jnp.where(good, pivot, 1.0), 0.0)

    i0 = inverse(n1, 0.0 * n1)
    l1, l2 = n2 * i0, n3 * i0
    d1, h = n3 - l1 * n2, n4 - l1 * n3
    i1 = inverse(d1, n3)
    l3 = h * i1
    d2 = n5 - l2 * n3 - l3 * h
    i2 = inverse(d2, n5)
    y1 = n1 - l1 * n0
    y2 = n2 - l2 * n0 - l3 * y1
    c2 = y2 * i2
    c1 = y1 * i1 - l3 * c2
    c0 = n0 * i0 - l1 * c1 - l2 * c2
    c0, c1, c2 = (jnp.broadcast_to(c, (1, width)) for c in (c0, c1, c2))

    def combine(k, carry):
        at = pl.multiple_of(k * 16, 16)
        inner_at = pl.multiple_of(HALO + k * 16, 8)
        part = pl.ds(inner_at, 16)
        x = c0 * w0[part, :] + c1 * w1[part, :] + c2 * w2[part, :]
        height[pl.ds(at, 16), :] = x
        warm = jnp.where(mask_ref[pl.ds(at, 16), :] == 1, temp_ref[pl.ds(at, 16), :] + x, 0.0).astype(BF16)
        for j in range(per):
            sst[pl.ds(pl.multiple_of(j * own + k * 16, 16), 16), :] = warm[:, j * LANES : (j + 1) * LANES]
        return carry

    lax.fori_loop(0, own // 16, combine, 0)
    height_copy = pltpu.make_async_copy(height, height_hbm, height_sem)
    height_copy.start()

    n_req = tiles * nrows
    at_once = min(256, n_req)

    def picked(i, carry):
        part = pl.ds(pl.multiple_of(i * at_once, at_once), at_once)
        rows_send[part, :] = jnp.dot(picks[part, :], sst[...], preferred_element_type=F32).astype(BF16)
        return carry

    lax.fori_loop(0, n_req // at_once, picked, 0)
    rows_slot = pl.ds(pl.multiple_of(tile * nrows, nrows), nrows)
    rows_recv[rows_slot, :] = rows_send[rows_slot, :]

    def rows_copy(i):
        other = lax.rem(tile + i, tiles)
        return pltpu.make_async_remote_copy(
            src_ref=rows_send.at[pl.ds(pl.multiple_of(other * nrows, nrows), nrows)],
            dst_ref=rows_recv.at[rows_slot],
            send_sem=rows_ssem.at[i],
            recv_sem=rows_rsem.at[i],
            device_id=(group, other),
            device_id_type=MESH,
        )

    each(rows_copy, start, 1, tiles)
    each(rows_copy, arrived, 1, tiles)
    got = jnp.sum(rows_recv[...].astype(F32).reshape(tiles, nrows, LANES), axis=0)
    for k in range(nrows):
        rows_out[:, k * LANES : (k + 1) * LANES] = got[k : k + 1, :]

    each(request, sent, 1, tiles)
    each(flux_copy, sent, 1, count)
    each(gram_copy, sent, 1, tiles)
    each(rows_copy, sent, 1, tiles)
    for i in range(n_chunk):
        store_pre(i).wait()
    height_copy.wait()


def solution(mesh):
    groups, tiles = mesh.shape["comp"], mesh.shape["tile"]
    count = groups * tiles

    def body(state, vco, weight, response, blocks, source, entry, present, mask, depth, temp, wanted):
        lev, cols = state.shape
        own, width = mask.shape
        nrows = cols // LANES
        n_flux = count * nrows
        n_ocean = own * width // LANES
        ext = own + 2 * HALO
        n_req = tiles * nrows
        n_chunk = max(1, cols // 1024)
        vmem = pl.BlockSpec(memory_space=pltpu.VMEM)
        anywhere = pl.BlockSpec(memory_space=pl.ANY)
        dma = pltpu.SemaphoreType.DMA
        asked = jnp.broadcast_to(jnp.pad(wanted, (0, LANES - nrows), constant_values=-1)[None, :], (8, LANES))
        pre, height, rows = pl.pallas_call(
            functools.partial(kernel, groups, tiles),
            out_shape=(
                jax.ShapeDtypeStruct((lev, cols), F32),
                jax.ShapeDtypeStruct((own, width), F32),
                jax.ShapeDtypeStruct((1, cols), F32),
            ),
            in_specs=[anywhere] + [vmem] * 10,
            out_specs=(anywhere, anywhere, vmem),
            scratch_shapes=[
                pltpu.VMEM((lev, cols), F32),
                pltpu.VMEM((2 * lev, 2 * lev), BF16),
                pltpu.VMEM((nrows, LANES), F32),
                pltpu.VMEM((n_flux, LANES), BF16),
                pltpu.VMEM((blocks.shape[0] * n_flux + 8, LANES), F32),
                pltpu.VMEM((4, n_ocean + 2 * LANES), I32),
                pltpu.SMEM((4, n_ocean + 2 * LANES), I32),
                pltpu.VMEM((ext, width), F32),
                pltpu.VMEM((ext, width), F32),
                pltpu.VMEM((ext, width), F32),
                pltpu.VMEM((ext, width), F32),
                pltpu.VMEM((ext, width), F32),
                pltpu.VMEM((own, width), F32),
                pltpu.VMEM((tiles * 8, LANES), I32),
                pltpu.VMEM((n_req, n_ocean), BF16),
                pltpu.VMEM((n_ocean, LANES), BF16),
                pltpu.VMEM((n_req, LANES), BF16),
                pltpu.VMEM((n_req, LANES), BF16),
                pltpu.VMEM((8, LANES), F32),
                pltpu.VMEM((tiles * 8, LANES), F32),
                dma((n_chunk,)),
                dma((n_chunk,)),
                dma,
                dma,
                dma((count,)),
                dma((count,)),
                dma((tiles,)),
                dma((tiles,)),
                dma((4,)),
                dma((4,)),
                dma((tiles,)),
                dma((tiles,)),
                dma((tiles,)),
                dma((tiles,)),
            ],
            compiler_params=pltpu.CompilerParams(
                collective_id=0, has_side_effects=True, vmem_limit_bytes=48 * 1024 * 1024
            ),
        )(
            state,
            vco,
            weight.reshape(lev, 1),
            blocks,
            source.T,
            entry.T,
            present.T,
            mask,
            depth,
            temp,
            asked,
        )
        return pre + (TIME_STEP * response)[:, None] * rows, height

    split = P(None, ("comp", "tile"))
    ocean = P("tile", None)
    return jax.shard_map(
        body,
        mesh=mesh,
        in_specs=(split, P(), P(), P(), P(), ocean, ocean, ocean, ocean, ocean, ocean, P(("comp", "tile"))),
        out_specs=(split, ocean),
        check_vma=False,
    )
```

```python
import functools

import jax
import jax.numpy as jnp
from jax import lax
from jax.experimental import pallas as pl
from jax.experimental.pallas import tpu as pltpu
from jax.sharding import PartitionSpec as P

F32, BF16, I32 = jnp.float32, jnp.bfloat16, jnp.int32
MESH = pl.DeviceIdType.MESH
LANES = 128
HALO = 8
TIME_STEP = 0.5


def kernel(
    groups,
    tiles,
    state_hbm,
    vco_hbm,
    weight_hbm,
    blocks_hbm,
    source_hbm,
    entry_hbm,
    present_hbm,
    mask_hbm,
    depth_hbm,
    temp_hbm,
    wanted_hbm,
    pre,
    height,
    rows_out,
    state,
    vco_ref,
    weight_ref,
    blocks_ref,
    source_ref,
    entry_ref,
    present_ref,
    mask_ref,
    depth_ref,
    temp_ref,
    wanted_ref,
    vv,
    fluxf,
    flux_all,
    table,
    idx_v,
    idx_s,
    coef,
    field,
    w0,
    w1,
    w2,
    req_v,
    picks,
    sst,
    rows_send,
    rows_recv,
    gram_send,
    gram_recv,
    in_sem,
    load_sem,
    idx_sem,
    flux_ssem,
    flux_rsem,
    fwd_ssem,
    fwd_rsem,
    req_ssem,
    req_rsem,
    halo_ssem,
    halo_rsem,
    gram_ssem,
    gram_rsem,
    rows_ssem,
    rows_rsem,
):
    group, tile = lax.axis_index("comp"), lax.axis_index("tile")
    count = groups * tiles
    lev, cols = state.shape
    own, width = mask_hbm.shape
    per = width // LANES
    ext = own + 2 * HALO
    nrows = cols // LANES
    n_flux = count * nrows
    n_entry, n_ocean = source_hbm.shape
    n_block = blocks_ref.shape[0]
    chunk = min(1024, cols)
    n_chunk = cols // chunk
    core, side = lax.rem(tile, 2), tiles // 2
    n_chip = groups * side
    chip = group * side + lax.div(tile, 2)
    partner = tile + 1 - 2 * core
    half = n_flux // 2
    part_rows = side * nrows
    span = n_ocean + 2 * LANES

    def chip_peer(i):
        other = lax.rem(chip + i, n_chip)
        return lax.div(other, side), 2 * lax.rem(other, side) + core

    loads = {
        name: pltpu.make_async_copy(source, target, load_sem.at[i])
        for i, (name, source, target) in enumerate(
            (
                ("vco", vco_hbm, vco_ref),
                ("weight", weight_hbm, weight_ref),
                ("mask", mask_hbm, mask_ref),
                ("depth", depth_hbm, depth_ref),
                ("source", source_hbm, source_ref),
                ("entry", entry_hbm, entry_ref),
                ("present", present_hbm, present_ref),
                ("wanted", wanted_hbm, wanted_ref),
                ("blocks", blocks_hbm, blocks_ref),
                ("temp", temp_hbm, temp_ref),
            )
        )
    }
    loads["vco"].start()

    def load_state(i):
        part = pl.ds(i * chunk, chunk)
        return pltpu.make_async_copy(state_hbm.at[:, part], state.at[:, part], in_sem.at[i])

    for i in range(n_chunk):
        load_state(i).start()

    barrier = pltpu.get_barrier_semaphore()

    def greet(target):
        pl.semaphore_signal(barrier, inc=1, device_id=target, device_id_type=MESH)

    def greet_chip(i, carry):
        greet(chip_peer(i))
        return carry

    def greet_other_core(i, carry):
        greet((group, 2 * i + 1 - core))
        return carry

    lax.fori_loop(1, n_chip, greet_chip, 0)
    lax.fori_loop(0, side, greet_other_core, 0)
    for name in loads:
        if name != "vco":
            loads[name].start()

    loads["vco"].wait()
    vco = vco_ref[...]
    v_hi = vco.astype(BF16)
    v_lo = (vco - v_hi.astype(F32)).astype(BF16)
    vv[0:lev, 0:lev] = v_hi
    vv[0:lev, lev : 2 * lev] = v_hi
    vv[lev : 2 * lev, 0:lev] = v_lo
    vv[lev : 2 * lev, lev : 2 * lev] = v_lo

    def tendency(s):
        hi = s.astype(BF16)
        lo = (s - hi.astype(F32)).astype(BF16)
        both = jnp.dot(vv[...], jnp.concatenate([hi, lo], axis=0), preferred_element_type=F32)
        return TIME_STEP * jnp.tanh(both[0:lev] + both[lev : 2 * lev])

    loads["weight"].wait()
    column = jnp.transpose(jnp.broadcast_to(weight_ref[...], (LANES, lev)))[:, 0:1]

    def first_steps(i):
        load_state(i).wait()
        part = pl.ds(i * chunk, chunk)
        s = state[:, part]
        s = s + tendency(s)
        s = s + tendency(s)
        state[:, part] = s
        line = jnp.sum(s * column, axis=0, keepdims=True)
        for k in range(chunk // LANES):
            fluxf[i * (chunk // LANES) + k : i * (chunk // LANES) + k + 1, :] = line[:, k * LANES : (k + 1) * LANES]

    for i in range(n_chunk - 1):
        first_steps(i)

    for name in ("mask", "depth", "source", "entry", "present", "wanted"):
        loads[name].wait()
    mask = mask_ref[...].astype(F32)
    coef[HALO : HALO + own, :] = mask * (4.0 + depth_ref[...])
    spare = n_block * n_flux
    source = source_ref[...]
    holder = lax.div(source, nrows)
    row = lax.rem(holder, 2) * half + lax.div(holder, 2) * nrows + lax.rem(source, nrows)
    index = jnp.where(present_ref[...] == 1, entry_ref[...] * n_flux + row, jnp.full(source.shape, spare, I32))
    for k in range(n_entry):
        idx_v[k, :, LANES : LANES + n_ocean] = index[k : k + 1, :]
    own_slot = pl.ds(pl.multiple_of(tile * 8, 8), 8)
    req_v[own_slot, :] = jnp.full((8, LANES), -1, I32)
    req_v[own_slot, 0:nrows] = jnp.broadcast_to(wanted_ref[...], (8, nrows))
    table[pl.ds(spare, 8), :] = jnp.zeros((8, LANES), F32)

    pl.semaphore_wait(barrier, n_chip - 1 + side)

    start = lambda c: c.start()

    def each(make, what, first, last):
        def step(i, carry):
            what(make(i))
            return carry

        lax.fori_loop(first, last, step, 0)

    def many(ref, rows, send_sem, recv_sem):
        return pltpu.make_async_remote_copy(
            src_ref=ref.at[pl.ds(0, rows)],
            dst_ref=ref.at[pl.ds(0, rows)],
            send_sem=send_sem,
            recv_sem=recv_sem,
            device_id=(group, partner),
            device_id_type=MESH,
        )

    def request(i):
        return pltpu.make_async_remote_copy(
            src_ref=req_v.at[own_slot],
            dst_ref=req_v.at[own_slot],
            send_sem=req_ssem,
            recv_sem=req_rsem,
            device_id=(group, lax.rem(tile + i, tiles)),
            device_id_type=MESH,
        )

    each(request, start, 1, tiles)
    requests = many(req_v, (tiles - 1) * 8, req_ssem, req_rsem)

    first_steps(n_chunk - 1)
    mine = pl.ds(pl.multiple_of(core * half + chip * nrows, nrows), nrows)
    flux_all[mine, :] = fluxf[...].astype(BF16)

    def flux_copy(i):
        return pltpu.make_async_remote_copy(
            src_ref=flux_all.at[mine],
            dst_ref=flux_all.at[mine],
            send_sem=flux_ssem,
            recv_sem=flux_rsem.at[group],
            device_id=chip_peer(i),
            device_id_type=MESH,
        )

    each(flux_copy, start, 1, n_chip)

    after, before = lax.rem(tile + 1, tiles), lax.rem(tile + tiles - 1, tiles)

    def halo(ref, src, dst, k, target):
        return pltpu.make_async_remote_copy(
            src_ref=ref.at[src],
            dst_ref=ref.at[dst],
            send_sem=halo_ssem.at[k],
            recv_sem=halo_rsem.at[k],
            device_id=(group, target),
            device_id_type=MESH,
        )

    everything = slice(None)
    halos = (
        halo(coef, (pl.ds(own, HALO), everything), (pl.ds(0, HALO), everything), 0, after),
        halo(coef, (pl.ds(HALO, HALO), everything), (pl.ds(HALO + own, HALO), everything), 1, before),
        halo(idx_v, (everything, everything, pl.ds(n_ocean, LANES)), (everything, everything, pl.ds(0, LANES)), 2, after),
        halo(
            idx_v,
            (everything, everything, pl.ds(LANES, LANES)),
            (everything, everything, pl.ds(LANES + n_ocean, LANES)),
            3,
            before,
        ),
    )
    for copy in halos:
        copy.start()

    for i in range(n_chunk):
        part = pl.ds(i * chunk, chunk)
        s = state[:, part]
        pre[:, part] = s + tendency(s)

    requests.wait_recv()
    asked = jnp.concatenate([req_v[8 * t : 8 * t + 1, :] for t in range(tiles)], axis=0)
    asked = jnp.concatenate([asked - tile * n_ocean, jnp.zeros((LANES - tiles, LANES), I32)], axis=0)
    asked = jnp.transpose(asked)
    where_col = lax.broadcasted_iota(I32, (nrows, n_ocean), 1)
    stacked = lax.rem(where_col, own) * per + lax.div(where_col, own)
    for t in range(tiles):
        hit = asked[0:nrows, t : t + 1] == stacked
        picks[t * nrows : (t + 1) * nrows, :] = jnp.where(hit, 1.0, 0.0).astype(BF16)

    loads["blocks"].wait()
    pairs = [jnp.concatenate([blocks_ref[b], blocks_ref[b + 1]], axis=1) for b in range(0, n_block, 2)]

    def products(at):
        some = flux_all[pl.ds(pl.multiple_of(at, part_rows), part_rows), :]
        for b, pair in enumerate(pairs):
            got = jnp.dot(some, pair, preferred_element_type=F32)
            for k in range(2):
                to = pl.multiple_of((2 * b + k) * n_flux + at, part_rows)
                table[pl.ds(to, part_rows), :] = got[:, k * LANES : (k + 1) * LANES]

    def forward(g):
        slot = pl.ds(pl.multiple_of(core * half + g * part_rows, part_rows), part_rows)
        return pltpu.make_async_remote_copy(
            src_ref=flux_all.at[slot],
            dst_ref=flux_all.at[slot],
            send_sem=fwd_ssem.at[g],
            recv_sem=fwd_rsem.at[g],
            device_id=(group, partner),
            device_id_type=MESH,
        )

    order = [0] + [k for n in range(1, groups // 2 + 1) for k in sorted({n, groups - n})]
    for n, offset in enumerate(order):
        g = lax.rem(group + offset, groups)
        blocks_in = side - 1 if offset == 0 else side
        many(flux_all, blocks_in * nrows, flux_ssem, flux_rsem.at[g]).wait_recv()
        forward(g).start()
        products(core * half + g * part_rows)
        if n > 0:
            late = lax.rem(group + order[n - 1], groups)
            forward(late).wait_recv()
            products((1 - core) * half + late * part_rows)
        if n == len(order) - 2:
            for copy in halos:
                copy.wait()
            index_copies = [
                pltpu.make_async_copy(
                    idx_v.at[k, 0], idx_s.at[pl.ds(k * span, span)], idx_sem.at[k]
                )
                for k in range(n_entry)
            ]
            for copy in index_copies:
                copy.start()
            inner = jnp.where(coef[...] > 0.0, 1.0 / coef[...], 0.0)
            coef[...] = inner
            coef[0:HALO, :] = jnp.where(tile > 0, inner[0:HALO], 0.0)
            coef[HALO + own : ext, :] = jnp.where(tile < tiles - 1, inner[HALO + own : ext], 0.0)
            zero_rows = jnp.zeros((HALO, width), F32)
            field[0:HALO, :] = zero_rows
            field[HALO + own : ext, :] = zero_rows
            for copy in index_copies:
                copy.wait()
    late = lax.rem(group + order[-1], groups)
    forward(late).wait_recv()
    products((1 - core) * half + late * part_rows)

    def forcing_rows(g_tile, j, rows):
        base = g_tile * 8 * per + j
        totals = []
        for s in rows:
            e = base + ((s - HALO) * per + LANES)
            got = [table[pl.ds(idx_s[e + k * span], 1), :] for k in range(n_entry)]
            while len(got) > 1:
                got = [sum(got[k : k + 2][1:], got[k]) for k in range(0, len(got), 2)]
            totals.append(got[0])
        at = pl.multiple_of(g_tile * 8, 8)
        block = field.at[pl.ds(at, 8), pl.ds(pl.multiple_of(j * LANES, LANES), LANES)]
        for s, total in zip(rows, totals):
            block[s : s + 1, :] = total

    def edge(j, carry):
        forcing_rows(0, j, (HALO - 3, HALO - 2, HALO - 1))
        forcing_rows(ext // 8 - 1, j, (0, 1, 2))
        return carry

    lax.fori_loop(0, per, edge, 0)

    def inside_rows(n, carry):
        forcing_rows(1 + lax.div(n, per), lax.rem(n, per), range(8))
        return carry

    lax.fori_loop(0, own // 8 * per, inside_rows, 0, unroll=2)

    n_tile = ext // 8
    top = lax.broadcasted_iota(I32, (8, width), 0) == 0
    bottom = lax.broadcasted_iota(I32, (8, width), 0) == 7

    def rows8(ref, k):
        return ref[pl.ds(pl.multiple_of(k * 8, 8), 8), :]

    def beside(ref, k):
        here = rows8(ref, k)
        above = rows8(ref, jnp.maximum(k - 1, 0))
        below = rows8(ref, jnp.minimum(k + 1, n_tile - 1))
        up = jnp.where(top, pltpu.roll(above, 1, 0), pltpu.roll(here, 1, 0))
        down = jnp.where(bottom, pltpu.roll(below, 7, 0), pltpu.roll(here, 7, 0))
        return up + down + pltpu.roll(here, 1, 1) + pltpu.roll(here, width - 1, 1)

    def folded(value):
        total = value[:, 0:LANES]
        for k in range(1, per):
            total = total + value[:, k * LANES : (k + 1) * LANES]
        return total

    nothing = jnp.zeros((8, LANES), F32)

    def first(k, carry):
        f = rows8(field, k)
        w = rows8(coef, k) * f
        w0[pl.ds(pl.multiple_of(k * 8, 8), 8), :] = w
        inside = jnp.logical_and(k >= 1, k < n_tile - 1)
        return carry + jnp.where(inside, folded(w * f), 0.0)

    nu0 = lax.fori_loop(0, n_tile, first, nothing, unroll=5)

    def apply(w_old, w_new, k, carry):
        a, b = carry
        q = rows8(field, k) - beside(w_old, k)
        w = rows8(coef, k) * q
        field[pl.ds(pl.multiple_of(k * 8, 8), 8), :] = q
        w_new[pl.ds(pl.multiple_of(k * 8, 8), 8), :] = w
        inside = jnp.logical_and(k >= 1, k < n_tile - 1)
        a = a + jnp.where(inside, folded(rows8(w_old, k) * q), 0.0)
        b = b + jnp.where(inside, folded(w * q), 0.0)
        return a, b

    nu1, nu2 = lax.fori_loop(0, n_tile, functools.partial(apply, w0, w1), (nothing, nothing), unroll=5)
    nu3, nu4 = lax.fori_loop(0, n_tile, functools.partial(apply, w1, w2), (nothing, nothing), unroll=5)

    def last(k, carry):
        q = rows8(field, k) - beside(w2, k)
        return carry + folded(rows8(w2, k) * q)

    nu5 = lax.fori_loop(1, n_tile - 1, last, nothing, unroll=4)

    gram_send[...] = jnp.zeros((8, LANES), F32)
    for k, nu in enumerate((nu0, nu1, nu2, nu3, nu4, nu5)):
        gram_send[k : k + 1, :] = jnp.sum(nu, axis=0, keepdims=True)
    gram_slot = pl.ds(pl.multiple_of(tile * 8, 8), 8)
    gram_recv[gram_slot, :] = gram_send[...]

    def gram_copy(i):
        return pltpu.make_async_remote_copy(
            src_ref=gram_send,
            dst_ref=gram_recv.at[gram_slot],
            send_sem=gram_ssem,
            recv_sem=gram_rsem,
            device_id=(group, lax.rem(tile + i, tiles)),
            device_id_type=MESH,
        )

    each(gram_copy, start, 1, tiles)
    gram_all = many(gram_recv, (tiles - 1) * 8, gram_ssem, gram_rsem)
    gram_all.wait_recv()
    total = jnp.sum(gram_recv[...].reshape(tiles, 8, LANES), axis=0)
    total = jnp.sum(total, axis=1, keepdims=True)
    n0, n1, n2, n3, n4, n5 = (total[k : k + 1, :] for k in range(6))

    def inverse(pivot, scale):
        good = pivot > 1e-6 * scale
        return jnp.where(good, 1.0 / jnp.where(good, pivot, 1.0), 0.0)

    i0 = inverse(n1, 0.0 * n1)
    l1, l2 = n2 * i0, n3 * i0
    d1, h = n3 - l1 * n2, n4 - l1 * n3
    i1 = inverse(d1, n3)
    l3 = h * i1
    d2 = n5 - l2 * n3 - l3 * h
    i2 = inverse(d2, n5)
    y1 = n1 - l1 * n0
    y2 = n2 - l2 * n0 - l3 * y1
    c2 = y2 * i2
    c1 = y1 * i1 - l3 * c2
    c0 = n0 * i0 - l1 * c1 - l2 * c2
    c0, c1, c2 = (jnp.broadcast_to(c, (1, width)) for c in (c0, c1, c2))

    def combine(k, carry):
        at = pl.multiple_of(k * 16, 16)
        inner_at = pl.multiple_of(HALO + k * 16, 8)
        part = pl.ds(inner_at, 16)
        x = c0 * w0[part, :] + c1 * w1[part, :] + c2 * w2[part, :]
        height[pl.ds(at, 16), :] = x
        warm = jnp.where(mask_ref[pl.ds(at, 16), :] == 1, temp_ref[pl.ds(at, 16), :] + x, 0.0).astype(BF16)
        for j in range(per):
            sst[pl.ds(pl.multiple_of(j * own + k * 16, 16), 16), :] = warm[:, j * LANES : (j + 1) * LANES]
        return carry

    loads["temp"].wait()
    lax.fori_loop(0, own // 16, combine, 0)

    n_req = tiles * nrows
    at_once = min(256, n_req)

    def picked(i, carry):
        part = pl.ds(pl.multiple_of(i * at_once, at_once), at_once)
        rows_send[part, :] = jnp.dot(picks[part, :], sst[...], preferred_element_type=F32).astype(BF16)
        return carry

    lax.fori_loop(0, n_req // at_once, picked, 0)
    rows_slot = pl.ds(pl.multiple_of(tile * nrows, nrows), nrows)
    rows_recv[rows_slot, :] = rows_send[rows_slot, :]

    def rows_copy(i):
        other = lax.rem(tile + i, tiles)
        return pltpu.make_async_remote_copy(
            src_ref=rows_send.at[pl.ds(pl.multiple_of(other * nrows, nrows), nrows)],
            dst_ref=rows_recv.at[rows_slot],
            send_sem=rows_ssem,
            recv_sem=rows_rsem,
            device_id=(group, other),
            device_id_type=MESH,
        )

    each(rows_copy, start, 1, tiles)
    rows_all = many(rows_recv, (tiles - 1) * nrows, rows_ssem, rows_rsem)
    rows_all.wait_recv()
    got = jnp.sum(rows_recv[...].astype(F32).reshape(tiles, nrows, LANES), axis=0)
    for k in range(nrows):
        rows_out[:, k * LANES : (k + 1) * LANES] = got[k : k + 1, :]

    requests.wait_send()
    many(flux_all, (n_chip - 1) * nrows, flux_ssem, flux_rsem.at[0]).wait_send()
    for g in range(groups):
        forward(g).wait_send()
    gram_all.wait_send()
    rows_all.wait_send()


def finish(pre, height, rows, response, atm_hbm, height_hbm, held, sems, height_sem):
    copy = pltpu.make_async_copy(height, height_hbm, height_sem)
    copy.start()
    lev, cols = pre.shape
    column = TIME_STEP * jnp.transpose(jnp.broadcast_to(response[...], (LANES, lev)))[:, 0:1]
    n_part = sems.shape[0]
    size = cols // n_part
    outs = []
    for i in range(n_part):
        part = pl.ds(i * size, size)
        held[:, part] = pre[:, part] + column * rows[:, part]
        outs.append(pltpu.make_async_copy(held.at[:, part], atm_hbm.at[:, part], sems.at[i]))
        outs[-1].start()
    for out in outs:
        out.wait()
    copy.wait()


def solution(mesh):
    groups, tiles = mesh.shape["comp"], mesh.shape["tile"]
    count = groups * tiles

    def body(state, vco, weight, response, blocks, source, entry, present, mask, depth, temp, wanted):
        lev, cols = state.shape
        own, width = mask.shape
        nrows = cols // LANES
        n_flux = count * nrows
        n_ocean = own * width // LANES
        ext = own + 2 * HALO
        n_req = tiles * nrows
        n_chunk = max(1, cols // 1024)
        vmem = pl.BlockSpec(memory_space=pltpu.VMEM)
        n_block, n_entry = blocks.shape[0], source.shape[1]
        anywhere = pl.BlockSpec(memory_space=pltpu.HBM)
        dma = pltpu.SemaphoreType.DMA
        pre, height, rows = pl.pallas_call(
            functools.partial(kernel, groups, tiles),
            out_shape=(
                jax.ShapeDtypeStruct((lev, cols), F32),
                jax.ShapeDtypeStruct((own, width), F32),
                jax.ShapeDtypeStruct((1, cols), F32),
            ),
            in_specs=[anywhere] * 11,
            out_specs=(vmem, vmem, vmem),
            scratch_shapes=[
                pltpu.VMEM((lev, cols), F32),
                pltpu.VMEM((lev, lev), F32),
                pltpu.VMEM((1, lev), F32),
                pltpu.VMEM((n_block, LANES, LANES), BF16),
                pltpu.VMEM((n_entry, n_ocean), I32),
                pltpu.VMEM((n_entry, n_ocean), I32),
                pltpu.VMEM((n_entry, n_ocean), I32),
                pltpu.VMEM((own, width), I32),
                pltpu.VMEM((own, width), F32),
                pltpu.VMEM((own, width), F32),
                pltpu.VMEM((1, nrows), I32),
                pltpu.VMEM((2 * lev, 2 * lev), BF16),
                pltpu.VMEM((nrows, LANES), F32),
                pltpu.VMEM((n_flux, LANES), BF16),
                pltpu.VMEM((n_block * n_flux + 8, LANES), F32),
                pltpu.VMEM((n_entry, 1, n_ocean + 2 * LANES), I32),
                pltpu.SMEM((n_entry * (n_ocean + 2 * LANES),), I32),
                pltpu.VMEM((ext, width), F32),
                pltpu.VMEM((ext, width), F32),
                pltpu.VMEM((ext, width), F32),
                pltpu.VMEM((ext, width), F32),
                pltpu.VMEM((ext, width), F32),
                pltpu.VMEM((tiles * 8, LANES), I32),
                pltpu.VMEM((n_req, n_ocean), BF16),
                pltpu.VMEM((n_ocean, LANES), BF16),
                pltpu.VMEM((n_req, LANES), BF16),
                pltpu.VMEM((n_req, LANES), BF16),
                pltpu.VMEM((8, LANES), F32),
                pltpu.VMEM((tiles * 8, LANES), F32),
                dma((n_chunk,)),
                dma((10,)),
                dma((n_entry,)),
                dma,
                dma((groups,)),
                dma((groups,)),
                dma((groups,)),
                dma,
                dma,
                dma((4,)),
                dma((4,)),
                dma,
                dma,
                dma,
                dma,
            ],
            compiler_params=pltpu.CompilerParams(
                collective_id=0, has_side_effects=True, vmem_limit_bytes=48 * 1024 * 1024
            ),
        )(
            *(
                pltpu.with_memory_space_constraint(value, pltpu.HBM)
                for value in (
                    state,
                    vco,
                    weight[None, :],
                    blocks,
                    source.T,
                    entry.T,
                    present.T,
                    mask,
                    depth,
                    temp,
                    wanted[None, :],
                )
            )
        )
        return pl.pallas_call(
            finish,
            out_shape=(jax.ShapeDtypeStruct((lev, cols), F32), jax.ShapeDtypeStruct((own, width), F32)),
            in_specs=[vmem] * 4,
            out_specs=(anywhere, anywhere),
            scratch_shapes=[pltpu.VMEM((lev, cols), F32), dma((n_chunk,)), dma],
            compiler_params=pltpu.CompilerParams(vmem_limit_bytes=16 * 1024 * 1024),
        )(pre, height, rows, response[None, :])

    split = P(None, ("comp", "tile"))
    ocean = P("tile", None)
    return jax.shard_map(
        body,
        mesh=mesh,
        in_specs=(split, P(), P(), P(), P(), ocean, ocean, ocean, ocean, ocean, ocean, P(("comp", "tile"))),
        out_specs=(split, ocean),
        check_vma=False,
    )
```

```python
import functools

import jax
import jax.numpy as jnp
from jax import lax
from jax.experimental import pallas as pl
from jax.experimental.pallas import tpu as pltpu
from jax.sharding import PartitionSpec as P

F32, BF16, I32 = jnp.float32, jnp.bfloat16, jnp.int32
MESH = pl.DeviceIdType.MESH
LANES = 128
HALO = 8
TIME_STEP = 0.5


FAR_FIRST = True


def hops(i, n):
    return min(i, n - i)


def kernel(
    groups,
    tiles,
    state_hbm,
    vco_hbm,
    weight_hbm,
    blocks_hbm,
    source_hbm,
    entry_hbm,
    present_hbm,
    mask_hbm,
    depth_hbm,
    temp_hbm,
    wanted_hbm,
    pre,
    height,
    rows_out,
    state,
    vco_ref,
    weight_ref,
    blocks_ref,
    source_ref,
    entry_ref,
    present_ref,
    mask_ref,
    depth_ref,
    temp_ref,
    wanted_ref,
    vv,
    fluxf,
    flux_all,
    table,
    idx_v,
    idx_s,
    coef,
    inv,
    field,
    w0,
    w1,
    w2,
    req_v,
    picks,
    sst,
    rows_send,
    rows_recv,
    gram_send,
    gram_recv,
    in_sem,
    load_sem,
    idx_sem,
    flux_ssem,
    flux_rsem,
    fwd_ssem,
    fwd_rsem,
    req_ssem,
    req_rsem,
    halo_ssem,
    halo_rsem,
    gram_ssem,
    gram_rsem,
    rows_ssem,
    rows_rsem,
):
    group, tile = lax.axis_index("comp"), lax.axis_index("tile")
    count = groups * tiles
    lev, cols = state.shape
    own, width = mask_hbm.shape
    per = width // LANES
    ext = own + 2 * HALO
    nrows = cols // LANES
    n_flux = count * nrows
    n_entry, n_ocean = source_hbm.shape
    n_block = blocks_ref.shape[0]
    chunk = min(1024, cols)
    n_chunk = cols // chunk
    core, side = lax.rem(tile, 2), tiles // 2
    n_chip = groups * side
    partner = tile + 1 - 2 * core
    half = n_flux // 2
    part_rows = side * nrows
    span = n_ocean + 2 * LANES

    lane_of_chip = lax.div(tile, 2)
    chip = group * side + lane_of_chip

    def around(value, size):
        return jnp.where(value >= size, value - size, value)

    def far_first(n):
        return sorted(range(n), key=lambda i: -min(i, n - i))

    wide = 4 if side % 4 == 0 else 1
    chip_order = [a * (side // wide) + b for a in far_first(wide) for b in far_first(side // wide)]
    chip_order.sort(key=lambda q: -(hops(q // (side // wide), wide) + hops(q % (side // wide), side // wide)))
    order = far_first(groups) if FAR_FIRST else far_first(groups)[::-1]

    def chip_peer(dg, dq):
        return around(group + dg, groups), 2 * around(lane_of_chip + dq, side) + core

    def tile_peer(dt):
        return group, around(tile + dt, tiles)

    chip_offsets = [(dg, dq) for dg in order for dq in chip_order if dg or dq]
    tile_offsets = [2 * dq + dc for dq in chip_order for dc in (0, 1) if dq or dc]

    loads = {
        name: pltpu.make_async_copy(source, target, load_sem.at[i])
        for i, (name, source, target) in enumerate(
            (
                ("vco", vco_hbm, vco_ref),
                ("weight", weight_hbm, weight_ref),
                ("mask", mask_hbm, mask_ref),
                ("depth", depth_hbm, depth_ref),
                ("source", source_hbm, source_ref),
                ("entry", entry_hbm, entry_ref),
                ("present", present_hbm, present_ref),
                ("wanted", wanted_hbm, wanted_ref),
                ("blocks", blocks_hbm, blocks_ref),
                ("temp", temp_hbm, temp_ref),
            )
        )
    }
    def load_state(i):
        part = pl.ds(i * chunk, chunk)
        return pltpu.make_async_copy(state_hbm.at[:, part], state.at[:, part], in_sem.at[i])

    loads["vco"].start()
    loads["weight"].start()
    for i in range(n_chunk):
        load_state(i).start()

    barrier = pltpu.get_barrier_semaphore()
    for target in [chip_peer(*d) for d in chip_offsets] + [
        (group, 2 * around(lane_of_chip + dq, side) + 1 - core) for dq in chip_order
    ]:
        pl.semaphore_signal(barrier, inc=1, device_id=target, device_id_type=MESH)
    for name in loads:
        if name not in ("vco", "weight"):
            loads[name].start()

    loads["vco"].wait()
    vco = vco_ref[...]
    v_hi = vco.astype(BF16)
    v_lo = (vco - v_hi.astype(F32)).astype(BF16)
    vv[0:lev, 0:lev] = v_hi
    vv[0:lev, lev : 2 * lev] = v_hi
    vv[lev : 2 * lev, 0:lev] = v_lo
    vv[lev : 2 * lev, lev : 2 * lev] = v_lo

    def tendency(s):
        hi = s.astype(BF16)
        lo = (s - hi.astype(F32)).astype(BF16)
        both = jnp.dot(vv[...], jnp.concatenate([hi, lo], axis=0), preferred_element_type=F32)
        return TIME_STEP * jnp.tanh(both[0:lev] + both[lev : 2 * lev])

    loads["weight"].wait()
    column = jnp.transpose(jnp.broadcast_to(weight_ref[...], (LANES, lev)))[:, 0:1]

    def first_steps(i):
        load_state(i).wait()
        part = pl.ds(i * chunk, chunk)
        s = state[:, part]
        s = s + tendency(s)
        s = s + tendency(s)
        state[:, part] = s
        line = jnp.sum(s * column, axis=0, keepdims=True)
        for k in range(chunk // LANES):
            fluxf[i * (chunk // LANES) + k : i * (chunk // LANES) + k + 1, :] = line[:, k * LANES : (k + 1) * LANES]

    for i in range(n_chunk):
        first_steps(i)
    mine = pl.ds(pl.multiple_of(core * half + chip * nrows, nrows), nrows)
    flux_all[mine, :] = fluxf[...].astype(BF16)

    for name in ("mask", "depth", "source", "entry", "present", "wanted"):
        loads[name].wait()
    mask = mask_ref[...].astype(F32)
    coef[HALO : HALO + own, :] = mask * (4.0 + depth_ref[...])
    spare = n_block * n_flux
    source = source_ref[...]
    holder = lax.div(source, nrows)
    row = lax.rem(holder, 2) * half + lax.div(holder, 2) * nrows + lax.rem(source, nrows)
    index = jnp.where(present_ref[...] == 1, entry_ref[...] * n_flux + row, jnp.full(source.shape, spare, I32))
    for k in range(n_entry):
        idx_v[k, :, LANES : LANES + n_ocean] = index[k : k + 1, :]
    own_slot = pl.ds(pl.multiple_of(tile * 8, 8), 8)
    req_v[own_slot, :] = jnp.full((8, LANES), -1, I32)
    req_v[own_slot, 0:nrows] = jnp.broadcast_to(wanted_ref[...], (8, nrows))
    table[pl.ds(spare, 8), :] = jnp.zeros((8, LANES), F32)

    pl.semaphore_wait(barrier, n_chip - 1 + side)

    def many(ref, rows, send_sem, recv_sem):
        return pltpu.make_async_remote_copy(
            src_ref=ref.at[pl.ds(0, rows)],
            dst_ref=ref.at[pl.ds(0, rows)],
            send_sem=send_sem,
            recv_sem=recv_sem,
            device_id=(group, partner),
            device_id_type=MESH,
        )

    def request(target):
        return pltpu.make_async_remote_copy(
            src_ref=req_v.at[own_slot],
            dst_ref=req_v.at[own_slot],
            send_sem=req_ssem,
            recv_sem=req_rsem,
            device_id=target,
            device_id_type=MESH,
        )

    for d in tile_offsets:
        request(tile_peer(d)).start()
    requests = many(req_v, (tiles - 1) * 8, req_ssem, req_rsem)

    def flux_copy(target):
        return pltpu.make_async_remote_copy(
            src_ref=flux_all.at[mine],
            dst_ref=flux_all.at[mine],
            send_sem=flux_ssem,
            recv_sem=flux_rsem.at[group],
            device_id=target,
            device_id_type=MESH,
        )

    for d in chip_offsets:
        flux_copy(chip_peer(*d)).start()

    after, before = lax.rem(tile + 1, tiles), lax.rem(tile + tiles - 1, tiles)

    def halo(ref, src, dst, k, target):
        return pltpu.make_async_remote_copy(
            src_ref=ref.at[src],
            dst_ref=ref.at[dst],
            send_sem=halo_ssem.at[k],
            recv_sem=halo_rsem.at[k],
            device_id=(group, target),
            device_id_type=MESH,
        )

    everything = slice(None)
    halos = (
        halo(coef, (pl.ds(own, HALO), everything), (pl.ds(0, HALO), everything), 0, after),
        halo(coef, (pl.ds(HALO, HALO), everything), (pl.ds(HALO + own, HALO), everything), 1, before),
        halo(idx_v, (everything, everything, pl.ds(n_ocean, LANES)), (everything, everything, pl.ds(0, LANES)), 2, after),
        halo(
            idx_v,
            (everything, everything, pl.ds(LANES, LANES)),
            (everything, everything, pl.ds(LANES + n_ocean, LANES)),
            3,
            before,
        ),
    )
    for copy in halos:
        copy.start()

    for i in range(n_chunk):
        part = pl.ds(i * chunk, chunk)
        s = state[:, part]
        pre[:, part] = s + tendency(s)

    zero_rows = jnp.zeros((HALO, width), F32)
    field[0:HALO, :] = zero_rows
    field[HALO + own : ext, :] = zero_rows

    def reciprocal(value):
        return jnp.where(value > 0.0, 1.0 / jnp.where(value > 0.0, value, 1.0), 0.0)

    inv[HALO : HALO + own, :] = reciprocal(coef[HALO : HALO + own, :])

    loads["blocks"].wait()
    pairs = [jnp.concatenate([blocks_ref[b], blocks_ref[b + 1]], axis=1) for b in range(0, n_block, 2)]

    def products(at):
        some = flux_all[pl.ds(pl.multiple_of(at, part_rows), part_rows), :]
        for b, pair in enumerate(pairs):
            got = jnp.dot(some, pair, preferred_element_type=F32)
            for k in range(2):
                to = pl.multiple_of((2 * b + k) * n_flux + at, part_rows)
                table[pl.ds(to, part_rows), :] = got[:, k * LANES : (k + 1) * LANES]

    def forward(g):
        slot = pl.ds(pl.multiple_of(core * half + g * part_rows, part_rows), part_rows)
        return pltpu.make_async_remote_copy(
            src_ref=flux_all.at[slot],
            dst_ref=flux_all.at[slot],
            send_sem=fwd_ssem.at[g],
            recv_sem=fwd_rsem.at[g],
            device_id=(group, partner),
            device_id_type=MESH,
        )

    for n, offset in enumerate(order):
        g = around(group + offset, groups)
        blocks_in = side - 1 if offset == 0 else side
        many(flux_all, blocks_in * nrows, flux_ssem, flux_rsem.at[g]).wait_recv()
        forward(g).start()
        if n > 0:
            late = around(group + order[n - 1], groups)
            forward(late).wait_recv()
            products((1 - core) * half + late * part_rows)
        products(core * half + g * part_rows)
        if n == len(order) - 2:
            for copy in halos:
                copy.wait()
            index_copies = [
                pltpu.make_async_copy(
                    idx_v.at[k, 0], idx_s.at[pl.ds(k * span, span)], idx_sem.at[k]
                )
                for k in range(n_entry)
            ]
            for copy in index_copies:
                copy.start()
            inv[0:HALO, :] = jnp.where(tile > 0, reciprocal(coef[0:HALO, :]), 0.0)
            inv[HALO + own : ext, :] = jnp.where(tile < tiles - 1, reciprocal(coef[HALO + own : ext, :]), 0.0)
    late = around(group + order[-1], groups)
    forward(late).wait_recv()
    products((1 - core) * half + late * part_rows)

    def forcing_rows(g_tile, j, rows):
        first_row = g_tile * 8 * per + j + (rows[0] - HALO) * per + LANES
        near = [idx_s.at[pl.ds(first_row + k * span, span)] for k in range(n_entry)]
        totals = []
        for s in rows:
            e = (s - rows[0]) * per
            got = [table[pl.ds(near[k][e], 1), :] for k in range(n_entry)]
            while len(got) > 1:
                got = [sum(got[k : k + 2][1:], got[k]) for k in range(0, len(got), 2)]
            totals.append(got[0])
        at = pl.multiple_of(g_tile * 8, 8)
        block = field.at[pl.ds(at, 8), pl.ds(pl.multiple_of(j * LANES, LANES), LANES)]
        for s, total in zip(rows, totals):
            block[s : s + 1, :] = total

    def edge(j, carry):
        forcing_rows(0, j, (HALO - 3, HALO - 2, HALO - 1))
        forcing_rows(ext // 8 - 1, j, (0, 1, 2))
        return carry

    for copy in index_copies:
        copy.wait()
    lax.fori_loop(0, per, edge, 0)

    def inside_rows(n, carry):
        forcing_rows(1 + lax.div(n, per), lax.rem(n, per), range(8))
        return carry

    lax.fori_loop(0, own // 8 * per, inside_rows, 0, unroll=2)

    n_tile = ext // 8
    top = lax.broadcasted_iota(I32, (8, width), 0) == 0
    bottom = lax.broadcasted_iota(I32, (8, width), 0) == 7

    def rows8(ref, k):
        return ref[pl.ds(pl.multiple_of(k * 8, 8), 8), :]

    def beside(ref, k):
        here = rows8(ref, k)
        above = rows8(ref, jnp.maximum(k - 1, 0))
        below = rows8(ref, jnp.minimum(k + 1, n_tile - 1))
        up = jnp.where(top, pltpu.roll(above, 1, 0), pltpu.roll(here, 1, 0))
        down = jnp.where(bottom, pltpu.roll(below, 7, 0), pltpu.roll(here, 7, 0))
        return up + down + pltpu.roll(here, 1, 1) + pltpu.roll(here, width - 1, 1)

    def folded(value):
        total = value[:, 0:LANES]
        for k in range(1, per):
            total = total + value[:, k * LANES : (k + 1) * LANES]
        return total

    nothing = jnp.zeros((8, LANES), F32)

    def first(k, carry):
        f = rows8(field, k)
        w = rows8(inv, k) * f
        w0[pl.ds(pl.multiple_of(k * 8, 8), 8), :] = w
        inside = jnp.logical_and(k >= 1, k < n_tile - 1)
        return carry + jnp.where(inside, folded(w * f), 0.0)

    nu0 = lax.fori_loop(0, n_tile, first, nothing, unroll=5)

    def apply(w_old, w_new, k, carry):
        a, b = carry
        q = rows8(field, k) - beside(w_old, k)
        w = rows8(inv, k) * q
        field[pl.ds(pl.multiple_of(k * 8, 8), 8), :] = q
        w_new[pl.ds(pl.multiple_of(k * 8, 8), 8), :] = w
        inside = jnp.logical_and(k >= 1, k < n_tile - 1)
        a = a + jnp.where(inside, folded(rows8(w_old, k) * q), 0.0)
        b = b + jnp.where(inside, folded(w * q), 0.0)
        return a, b

    nu1, nu2 = lax.fori_loop(0, n_tile, functools.partial(apply, w0, w1), (nothing, nothing), unroll=5)
    nu3, nu4 = lax.fori_loop(0, n_tile, functools.partial(apply, w1, w2), (nothing, nothing), unroll=5)

    def last(k, carry):
        q = rows8(field, k) - beside(w2, k)
        return carry + folded(rows8(w2, k) * q)

    nu5 = lax.fori_loop(1, n_tile - 1, last, nothing, unroll=4)

    gram_send[...] = jnp.zeros((8, LANES), F32)
    for k, nu in enumerate((nu0, nu1, nu2, nu3, nu4, nu5)):
        gram_send[k : k + 1, :] = jnp.sum(nu, axis=0, keepdims=True)
    gram_slot = pl.ds(pl.multiple_of(tile * 8, 8), 8)
    gram_recv[gram_slot, :] = gram_send[...]

    def gram_copy(target):
        return pltpu.make_async_remote_copy(
            src_ref=gram_send,
            dst_ref=gram_recv.at[gram_slot],
            send_sem=gram_ssem,
            recv_sem=gram_rsem,
            device_id=target,
            device_id_type=MESH,
        )

    for d in tile_offsets:
        gram_copy(tile_peer(d)).start()
    requests.wait_recv()
    asked = jnp.concatenate([req_v[8 * t : 8 * t + 1, :] for t in range(tiles)], axis=0)
    asked = jnp.concatenate([asked - tile * n_ocean, jnp.zeros((LANES - tiles, LANES), I32)], axis=0)
    asked = jnp.transpose(asked)
    where_col = lax.broadcasted_iota(I32, (nrows, n_ocean), 1)
    stacked = lax.rem(where_col, own) * per + lax.div(where_col, own)
    for t in range(tiles):
        hit = asked[0:nrows, t : t + 1] == stacked
        picks[t * nrows : (t + 1) * nrows, :] = jnp.where(hit, 1.0, 0.0).astype(BF16)

    gram_all = many(gram_recv, (tiles - 1) * 8, gram_ssem, gram_rsem)
    gram_all.wait_recv()
    total = jnp.sum(gram_recv[...].reshape(tiles, 8, LANES), axis=0)
    total = jnp.sum(total, axis=1, keepdims=True)
    n0, n1, n2, n3, n4, n5 = (total[k : k + 1, :] for k in range(6))

    def inverse(pivot, scale):
        good = pivot > 1e-6 * scale
        return jnp.where(good, 1.0 / jnp.where(good, pivot, 1.0), 0.0)

    i0 = inverse(n1, 0.0 * n1)
    l1, l2 = n2 * i0, n3 * i0
    d1, h = n3 - l1 * n2, n4 - l1 * n3
    i1 = inverse(d1, n3)
    l3 = h * i1
    d2 = n5 - l2 * n3 - l3 * h
    i2 = inverse(d2, n5)
    y1 = n1 - l1 * n0
    y2 = n2 - l2 * n0 - l3 * y1
    c2 = y2 * i2
    c1 = y1 * i1 - l3 * c2
    c0 = n0 * i0 - l1 * c1 - l2 * c2
    c0, c1, c2 = (jnp.broadcast_to(c, (1, width)) for c in (c0, c1, c2))

    def combine(k, carry):
        at = pl.multiple_of(k * 16, 16)
        inner_at = pl.multiple_of(HALO + k * 16, 8)
        part = pl.ds(inner_at, 16)
        x = c0 * w0[part, :] + c1 * w1[part, :] + c2 * w2[part, :]
        height[pl.ds(at, 16), :] = x
        warm = jnp.where(mask_ref[pl.ds(at, 16), :] == 1, temp_ref[pl.ds(at, 16), :] + x, 0.0).astype(BF16)
        for j in range(per):
            sst[pl.ds(pl.multiple_of(j * own + k * 16, 16), 16), :] = warm[:, j * LANES : (j + 1) * LANES]
        return carry

    loads["temp"].wait()
    lax.fori_loop(0, own // 16, combine, 0)

    rows_slot = pl.ds(pl.multiple_of(tile * nrows, nrows), nrows)
    wide_tiles = tiles // wide
    plane = lax.div(tile, wide_tiles)

    def rows_copy(other):
        return pltpu.make_async_remote_copy(
            src_ref=rows_send.at[pl.ds(pl.multiple_of(other * nrows, nrows), nrows)],
            dst_ref=rows_recv.at[rows_slot],
            send_sem=rows_ssem,
            recv_sem=rows_rsem,
            device_id=(group, other),
            device_id_type=MESH,
        )

    within = lax.rem(tile, wide_tiles)
    for dp in far_first(wide):
        goal = around(plane + dp, wide) * wide_tiles
        part = pl.ds(pl.multiple_of(goal * nrows, wide_tiles * nrows), wide_tiles * nrows)
        rows_send[part, :] = jnp.dot(picks[part, :], sst[...], preferred_element_type=F32).astype(BF16)
        for dt in far_first(wide_tiles):
            if dp or dt:
                rows_copy(goal + around(within + dt, wide_tiles)).start()
    rows_recv[rows_slot, :] = rows_send[rows_slot, :]
    rows_all = many(rows_recv, (tiles - 1) * nrows, rows_ssem, rows_rsem)
    rows_all.wait_recv()
    got = jnp.sum(rows_recv[...].astype(F32).reshape(tiles, nrows, LANES), axis=0)
    for k in range(nrows):
        rows_out[:, k * LANES : (k + 1) * LANES] = got[k : k + 1, :]

    requests.wait_send()
    many(flux_all, (n_chip - 1) * nrows, flux_ssem, flux_rsem.at[0]).wait_send()
    for g in range(groups):
        forward(g).wait_send()
    gram_all.wait_send()
    rows_all.wait_send()


def finish(pre, height, rows, response, atm_hbm, height_hbm, held, sems, height_sem):
    copy = pltpu.make_async_copy(height, height_hbm, height_sem)
    copy.start()
    lev, cols = pre.shape
    column = TIME_STEP * jnp.transpose(jnp.broadcast_to(response[...], (LANES, lev)))[:, 0:1]
    n_part = sems.shape[0]
    size = cols // n_part
    outs = []
    for i in range(n_part):
        part = pl.ds(i * size, size)
        held[:, part] = pre[:, part] + column * rows[:, part]
        outs.append(pltpu.make_async_copy(held.at[:, part], atm_hbm.at[:, part], sems.at[i]))
        outs[-1].start()
    for out in outs:
        out.wait()
    copy.wait()


def solution(mesh):
    groups, tiles = mesh.shape["comp"], mesh.shape["tile"]
    count = groups * tiles

    def body(state, vco, weight, response, blocks, source, entry, present, mask, depth, temp, wanted):
        lev, cols = state.shape
        own, width = mask.shape
        nrows = cols // LANES
        n_flux = count * nrows
        n_ocean = own * width // LANES
        ext = own + 2 * HALO
        n_req = tiles * nrows
        n_chunk = max(1, cols // 1024)
        vmem = pl.BlockSpec(memory_space=pltpu.VMEM)
        n_block, n_entry = blocks.shape[0], source.shape[1]
        anywhere = pl.BlockSpec(memory_space=pltpu.HBM)
        dma = pltpu.SemaphoreType.DMA
        pre, height, rows = pl.pallas_call(
            functools.partial(kernel, groups, tiles),
            out_shape=(
                jax.ShapeDtypeStruct((lev, cols), F32),
                jax.ShapeDtypeStruct((own, width), F32),
                jax.ShapeDtypeStruct((1, cols), F32),
            ),
            in_specs=[anywhere] * 11,
            out_specs=(vmem, vmem, vmem),
            scratch_shapes=[
                pltpu.VMEM((lev, cols), F32),
                pltpu.VMEM((lev, lev), F32),
                pltpu.VMEM((1, lev), F32),
                pltpu.VMEM((n_block, LANES, LANES), BF16),
                pltpu.VMEM((n_entry, n_ocean), I32),
                pltpu.VMEM((n_entry, n_ocean), I32),
                pltpu.VMEM((n_entry, n_ocean), I32),
                pltpu.VMEM((own, width), I32),
                pltpu.VMEM((own, width), F32),
                pltpu.VMEM((own, width), F32),
                pltpu.VMEM((1, nrows), I32),
                pltpu.VMEM((2 * lev, 2 * lev), BF16),
                pltpu.VMEM((nrows, LANES), F32),
                pltpu.VMEM((n_flux, LANES), BF16),
                pltpu.VMEM((n_block * n_flux + 8, LANES), F32),
                pltpu.VMEM((n_entry, 1, n_ocean + 2 * LANES), I32),
                pltpu.SMEM(((n_entry + 1) * (n_ocean + 2 * LANES),), I32),
                pltpu.VMEM((ext, width), F32),
                pltpu.VMEM((ext, width), F32),
                pltpu.VMEM((ext, width), F32),
                pltpu.VMEM((ext, width), F32),
                pltpu.VMEM((ext, width), F32),
                pltpu.VMEM((ext, width), F32),
                pltpu.VMEM((tiles * 8, LANES), I32),
                pltpu.VMEM((n_req, n_ocean), BF16),
                pltpu.VMEM((n_ocean, LANES), BF16),
                pltpu.VMEM((n_req, LANES), BF16),
                pltpu.VMEM((n_req, LANES), BF16),
                pltpu.VMEM((8, LANES), F32),
                pltpu.VMEM((tiles * 8, LANES), F32),
                dma((n_chunk,)),
                dma((10,)),
                dma((n_entry,)),
                dma,
                dma((groups,)),
                dma((groups,)),
                dma((groups,)),
                dma,
                dma,
                dma((4,)),
                dma((4,)),
                dma,
                dma,
                dma,
                dma,
            ],
            compiler_params=pltpu.CompilerParams(
                collective_id=0, has_side_effects=True, vmem_limit_bytes=48 * 1024 * 1024
            ),
        )(
            *(
                pltpu.with_memory_space_constraint(value, pltpu.HBM)
                for value in (
                    state,
                    vco,
                    weight[None, :],
                    blocks,
                    source.T,
                    entry.T,
                    present.T,
                    mask,
                    depth,
                    temp,
                    wanted[None, :],
                )
            )
        )
        return pl.pallas_call(
            finish,
            out_shape=(jax.ShapeDtypeStruct((lev, cols), F32), jax.ShapeDtypeStruct((own, width), F32)),
            in_specs=[vmem] * 4,
            out_specs=(anywhere, anywhere),
            scratch_shapes=[pltpu.VMEM((lev, cols), F32), dma((n_chunk,)), dma],
            compiler_params=pltpu.CompilerParams(vmem_limit_bytes=16 * 1024 * 1024),
        )(pre, height, rows, response[None, :])

    split = P(None, ("comp", "tile"))
    ocean = P("tile", None)
    return jax.shard_map(
        body,
        mesh=mesh,
        in_specs=(split, P(), P(), P(), P(), ocean, ocean, ocean, ocean, ocean, ocean, P(("comp", "tile"))),
        out_specs=(split, ocean),
        check_vma=False,
    )
```

```python
import functools

import jax
import jax.numpy as jnp
from jax import lax
from jax.experimental import pallas as pl
from jax.experimental.pallas import tpu as pltpu
from jax.sharding import PartitionSpec as P

F32, BF16, I32 = jnp.float32, jnp.bfloat16, jnp.int32
MESH = pl.DeviceIdType.MESH
LANES = 128
HALO = 8
TIME_STEP = 0.5


FAR_FIRST = True


def hops(i, n):
    return min(i, n - i)


def kernel(
    groups,
    tiles,
    state_hbm,
    vco_hbm,
    weight_hbm,
    blocks_hbm,
    source_hbm,
    entry_hbm,
    present_hbm,
    mask_hbm,
    depth_hbm,
    temp_hbm,
    wanted_hbm,
    response_hbm,
    pre,
    height,
    rows_out,
    column_out,
    state,
    vco_ref,
    weight_ref,
    blocks_ref,
    source_ref,
    entry_ref,
    present_ref,
    mask_ref,
    depth_ref,
    temp_ref,
    wanted_ref,
    response_ref,
    vv,
    fluxf,
    flux_all,
    table,
    idx_v,
    idx_s,
    coef,
    inv,
    field,
    w0,
    w1,
    w2,
    req_v,
    picks,
    sst,
    rows_send,
    rows_recv,
    gram_send,
    gram_recv,
    in_sem,
    load_sem,
    idx_sem,
    flux_ssem,
    flux_rsem,
    fwd_ssem,
    fwd_rsem,
    req_ssem,
    req_rsem,
    halo_ssem,
    halo_rsem,
    gram_ssem,
    gram_rsem,
    rows_ssem,
    rows_rsem,
):
    group, tile = lax.axis_index("comp"), lax.axis_index("tile")
    count = groups * tiles
    lev, cols = state.shape
    own, width = mask_hbm.shape
    per = width // LANES
    ext = own + 2 * HALO
    nrows = cols // LANES
    n_flux = count * nrows
    n_entry, n_ocean = source_hbm.shape
    n_block = blocks_ref.shape[0]
    chunk = min(1024, cols)
    n_chunk = cols // chunk
    core, side = lax.rem(tile, 2), tiles // 2
    n_chip = groups * side
    partner = tile + 1 - 2 * core
    half = n_flux // 2
    part_rows = side * nrows
    span = n_ocean + 2 * LANES

    lane_of_chip = lax.div(tile, 2)
    chip = group * side + lane_of_chip

    def around(value, size):
        return jnp.where(value >= size, value - size, value)

    def far_first(n):
        return sorted(range(n), key=lambda i: -min(i, n - i))

    wide = 4 if side % 4 == 0 else 1
    chip_order = [a * (side // wide) + b for a in far_first(wide) for b in far_first(side // wide)]
    chip_order.sort(key=lambda q: -(hops(q // (side // wide), wide) + hops(q % (side // wide), side // wide)))
    order = far_first(groups) if FAR_FIRST else far_first(groups)[::-1]

    def chip_peer(dg, dq):
        return around(group + dg, groups), 2 * around(lane_of_chip + dq, side) + core

    def tile_peer(dt):
        return group, around(tile + dt, tiles)

    chip_offsets = [(dg, dq) for dg in order for dq in chip_order if dg or dq]
    tile_offsets = [2 * dq + dc for dq in chip_order for dc in (0, 1) if dq or dc]

    loads = {
        name: pltpu.make_async_copy(source, target, load_sem.at[i])
        for i, (name, source, target) in enumerate(
            (
                ("vco", vco_hbm, vco_ref),
                ("weight", weight_hbm, weight_ref),
                ("mask", mask_hbm, mask_ref),
                ("depth", depth_hbm, depth_ref),
                ("source", source_hbm, source_ref),
                ("entry", entry_hbm, entry_ref),
                ("present", present_hbm, present_ref),
                ("wanted", wanted_hbm, wanted_ref),
                ("blocks", blocks_hbm, blocks_ref),
                ("temp", temp_hbm, temp_ref),
                ("response", response_hbm, response_ref),
            )
        )
    }

    def load_state(i):
        part = pl.ds(i * chunk, chunk)
        return pltpu.make_async_copy(state_hbm.at[:, part], state.at[:, part], in_sem.at[i])

    barrier = pltpu.get_barrier_semaphore()
    greeted = [chip_peer(*d) for d in chip_offsets]
    greeted += [(group, 2 * around(lane_of_chip + dq, side) + 1 - core) for dq in chip_order]

    def greet(targets):
        for target in targets:
            pl.semaphore_signal(barrier, inc=1, device_id=target, device_id_type=MESH)

    loads["vco"].start()
    for i in range(n_chunk):
        load_state(i).start()
    greet(greeted)
    loads["weight"].start()
    for name in loads:
        if name not in ("vco", "weight"):
            loads[name].start()

    loads["vco"].wait()
    vco = vco_ref[...]
    v_hi = vco.astype(BF16)
    v_lo = (vco - v_hi.astype(F32)).astype(BF16)
    vv[0:lev, 0:lev] = v_hi
    vv[0:lev, lev : 2 * lev] = v_hi
    vv[lev : 2 * lev, 0:lev] = v_lo
    vv[lev : 2 * lev, lev : 2 * lev] = v_lo

    def tendency(s):
        hi = s.astype(BF16)
        lo = (s - hi.astype(F32)).astype(BF16)
        both = jnp.dot(vv[...], jnp.concatenate([hi, lo], axis=0), preferred_element_type=F32)
        return TIME_STEP * jnp.tanh(both[0:lev] + both[lev : 2 * lev])

    for i in range(n_chunk):
        load_state(i).wait()
    loads["weight"].wait()
    column = jnp.transpose(jnp.broadcast_to(weight_ref[...], (LANES, lev)))[:, 0:1]
    parts = [pl.ds(i * chunk, chunk) for i in range(n_chunk)]
    for part in parts:
        s = state[:, part]
        state[:, part] = s + tendency(s)
    for i, part in enumerate(parts):
        s = state[:, part]
        s = s + tendency(s)
        state[:, part] = s
        line = jnp.sum(s * column, axis=0, keepdims=True)
        for k in range(chunk // LANES):
            fluxf[i * (chunk // LANES) + k : i * (chunk // LANES) + k + 1, :] = line[:, k * LANES : (k + 1) * LANES]
    mine = pl.ds(pl.multiple_of(core * half + chip * nrows, nrows), nrows)
    flux_all[mine, :] = fluxf[...].astype(BF16)

    pl.semaphore_wait(barrier, n_chip - 1 + side)

    def many(ref, rows, send_sem, recv_sem):
        return pltpu.make_async_remote_copy(
            src_ref=ref.at[pl.ds(0, rows)],
            dst_ref=ref.at[pl.ds(0, rows)],
            send_sem=send_sem,
            recv_sem=recv_sem,
            device_id=(group, partner),
            device_id_type=MESH,
        )

    def flux_copy(target):
        return pltpu.make_async_remote_copy(
            src_ref=flux_all.at[mine],
            dst_ref=flux_all.at[mine],
            send_sem=flux_ssem,
            recv_sem=flux_rsem.at[group],
            device_id=target,
            device_id_type=MESH,
        )

    for d in chip_offsets:
        flux_copy(chip_peer(*d)).start()

    for name in ("mask", "depth", "source", "entry", "present", "wanted"):
        loads[name].wait()
    mask = mask_ref[...].astype(F32)
    coef[HALO : HALO + own, :] = mask * (4.0 + depth_ref[...])
    spare = n_block * n_flux
    source = source_ref[...]
    holder = lax.div(source, nrows)
    row = lax.rem(holder, 2) * half + lax.div(holder, 2) * nrows + lax.rem(source, nrows)
    index = jnp.where(present_ref[...] == 1, entry_ref[...] * n_flux + row, jnp.full(source.shape, spare, I32))
    for k in range(n_entry):
        idx_v[k, :, LANES : LANES + n_ocean] = index[k : k + 1, :]
    own_slot = pl.ds(pl.multiple_of(tile * 8, 8), 8)
    req_v[own_slot, :] = jnp.full((8, LANES), -1, I32)
    req_v[own_slot, 0:nrows] = jnp.broadcast_to(wanted_ref[...], (8, nrows))
    table[pl.ds(spare, 8), :] = jnp.zeros((8, LANES), F32)

    def request(target):
        return pltpu.make_async_remote_copy(
            src_ref=req_v.at[own_slot],
            dst_ref=req_v.at[own_slot],
            send_sem=req_ssem,
            recv_sem=req_rsem,
            device_id=target,
            device_id_type=MESH,
        )

    for d in tile_offsets:
        request(tile_peer(d)).start()
    requests = many(req_v, (tiles - 1) * 8, req_ssem, req_rsem)

    after, before = lax.rem(tile + 1, tiles), lax.rem(tile + tiles - 1, tiles)

    def halo(ref, src, dst, k, target):
        return pltpu.make_async_remote_copy(
            src_ref=ref.at[src],
            dst_ref=ref.at[dst],
            send_sem=halo_ssem.at[k],
            recv_sem=halo_rsem.at[k],
            device_id=(group, target),
            device_id_type=MESH,
        )

    everything = slice(None)
    halos = (
        halo(coef, (pl.ds(own, HALO), everything), (pl.ds(0, HALO), everything), 0, after),
        halo(coef, (pl.ds(HALO, HALO), everything), (pl.ds(HALO + own, HALO), everything), 1, before),
        halo(idx_v, (everything, everything, pl.ds(n_ocean, LANES)), (everything, everything, pl.ds(0, LANES)), 2, after),
        halo(
            idx_v,
            (everything, everything, pl.ds(LANES, LANES)),
            (everything, everything, pl.ds(LANES + n_ocean, LANES)),
            3,
            before,
        ),
    )
    for copy in halos:
        copy.start()

    for i in range(n_chunk):
        part = pl.ds(i * chunk, chunk)
        s = state[:, part]
        pre[:, part] = s + tendency(s)

    loads["response"].wait()
    column_out[...] = TIME_STEP * jnp.transpose(jnp.broadcast_to(response_ref[...], (LANES, lev)))

    zero_rows = jnp.zeros((per, HALO, LANES), F32)
    field[:, 0:HALO, :] = zero_rows
    field[:, HALO + own : ext, :] = zero_rows

    def reciprocal(value):
        return jnp.where(value > 0.0, 1.0 / jnp.where(value > 0.0, value, 1.0), 0.0)

    def set_inverse(first, last, exists):
        for j in range(per):
            value = reciprocal(coef[first:last, j * LANES : (j + 1) * LANES])
            inv[j, first:last, :] = value if exists is None else jnp.where(exists, value, 0.0)

    set_inverse(HALO, HALO + own, None)

    loads["blocks"].wait()
    pairs = [jnp.concatenate([blocks_ref[b], blocks_ref[b + 1]], axis=1) for b in range(0, n_block, 2)]

    def products(at):
        some = flux_all[pl.ds(pl.multiple_of(at, part_rows), part_rows), :]
        for b, pair in enumerate(pairs):
            got = jnp.dot(some, pair, preferred_element_type=F32)
            for k in range(2):
                to = pl.multiple_of((2 * b + k) * n_flux + at, part_rows)
                table[pl.ds(to, part_rows), :] = got[:, k * LANES : (k + 1) * LANES]

    def forward(g):
        slot = pl.ds(pl.multiple_of(core * half + g * part_rows, part_rows), part_rows)
        return pltpu.make_async_remote_copy(
            src_ref=flux_all.at[slot],
            dst_ref=flux_all.at[slot],
            send_sem=fwd_ssem.at[g],
            recv_sem=fwd_rsem.at[g],
            device_id=(group, partner),
            device_id_type=MESH,
        )

    def take(offset):
        g = around(group + offset, groups)
        blocks_in = side - 1 if offset == 0 else side
        many(flux_all, blocks_in * nrows, flux_ssem, flux_rsem.at[g]).wait_recv()
        forward(g).start()

    def near(offset):
        products(core * half + around(group + offset, groups) * part_rows)

    def far(offset):
        products((1 - core) * half + around(group + offset, groups) * part_rows)

    def shared(offset):
        forward(around(group + offset, groups)).wait_recv()

    take(order[0])
    near(order[0])
    take(order[1])
    shared(order[0])
    near(order[1])
    far(order[0])
    for offset in order[2:]:
        take(offset)
    shared(order[1])
    for offset in order[2:]:
        near(offset)
    far(order[1])
    for copy in halos:
        copy.wait()
    index_copies = [
        pltpu.make_async_copy(idx_v.at[k, 0], idx_s.at[pl.ds(k * span, span)], idx_sem.at[k]) for k in range(n_entry)
    ]
    for copy in index_copies:
        copy.start()
    set_inverse(0, HALO, tile > 0)
    set_inverse(HALO + own, ext, tile < tiles - 1)
    for offset in order[2:]:
        shared(offset)
    for offset in order[2:]:
        far(offset)

    def forcing_rows(g_tile, j, rows):
        first_row = g_tile * 8 * per + j + (rows[0] - HALO) * per + LANES
        totals = []
        for s in rows:
            e = first_row + (s - rows[0]) * per
            got = [table[pl.ds(idx_s.at[pl.ds(e + k * span, 1)][0], 1), :] for k in range(n_entry)]
            while len(got) > 1:
                got = [sum(got[k : k + 2][1:], got[k]) for k in range(0, len(got), 2)]
            totals.append(got[0])
        at = pl.multiple_of(g_tile * 8, 8)
        block = field.at[j, pl.ds(at, 8), :]
        for s, total in zip(rows, totals):
            block[s : s + 1, :] = total

    def edge(j, carry):
        forcing_rows(0, j, (HALO - 3, HALO - 2, HALO - 1))
        forcing_rows(ext // 8 - 1, j, (0, 1, 2))
        return carry

    for copy in index_copies:
        copy.wait()
    lax.fori_loop(0, per, edge, 0)

    def inside_rows(g_tile, carry):
        def one(j, inner):
            forcing_rows(g_tile, j, range(8))
            return inner

        return lax.fori_loop(0, per, one, carry, unroll=5)

    lax.fori_loop(1, 1 + own // 8, inside_rows, 0)

    n_tile = ext // 8
    lane = lax.broadcasted_iota(I32, (per, 8, LANES), 2)

    def rows8(ref, k):
        return ref[:, 8 * k : 8 * k + 8, :]

    def beside(ref, k):
        here = rows8(ref, k)
        up = ref[:, 8 * k - 1 : 8 * k + 7, :] if k > 0 else pltpu.roll(here, 1, 1)
        down = ref[:, 8 * k + 1 : 8 * k + 9, :] if k < n_tile - 1 else pltpu.roll(here, 7, 1)
        one, other = pltpu.roll(here, 1, 2), pltpu.roll(here, LANES - 1, 2)
        left = jnp.where(lane == 0, jnp.concatenate([one[per - 1 :], one[: per - 1]], axis=0), one)
        right = jnp.where(lane == LANES - 1, jnp.concatenate([other[1:], other[:1]], axis=0), other)
        return (up + down) + (left + right)

    nothing = jnp.zeros((8, LANES), F32)
    own_tiles = range(1, n_tile - 1)

    nu0 = nothing
    for k in range(n_tile):
        f = rows8(field, k)
        w = rows8(inv, k) * f
        w0[:, 8 * k : 8 * k + 8, :] = w
        if k in own_tiles:
            nu0 = nu0 + jnp.sum(w * f, axis=0)

    def apply(w_old, w_new):
        a, b = nothing, nothing
        for k in range(n_tile):
            q = rows8(field, k) - beside(w_old, k)
            w = rows8(inv, k) * q
            field[:, 8 * k : 8 * k + 8, :] = q
            w_new[:, 8 * k : 8 * k + 8, :] = w
            if k in own_tiles:
                a = a + jnp.sum(rows8(w_old, k) * q, axis=0)
                b = b + jnp.sum(w * q, axis=0)
        return a, b

    nu1, nu2 = apply(w0, w1)
    nu3, nu4 = apply(w1, w2)
    nu5 = nothing
    for k in own_tiles:
        nu5 = nu5 + jnp.sum(rows8(w2, k) * (rows8(field, k) - beside(w2, k)), axis=0)

    gram_send[...] = jnp.zeros((8, LANES), F32)
    for k, nu in enumerate((nu0, nu1, nu2, nu3, nu4, nu5)):
        gram_send[k : k + 1, :] = jnp.sum(nu, axis=0, keepdims=True)
    gram_slot = pl.ds(pl.multiple_of(tile * 8, 8), 8)
    gram_recv[gram_slot, :] = gram_send[...]

    def gram_copy(target):
        return pltpu.make_async_remote_copy(
            src_ref=gram_send,
            dst_ref=gram_recv.at[gram_slot],
            send_sem=gram_ssem,
            recv_sem=gram_rsem,
            device_id=target,
            device_id_type=MESH,
        )

    for d in tile_offsets:
        gram_copy(tile_peer(d)).start()
    requests.wait_recv()
    asked = jnp.concatenate([req_v[8 * t : 8 * t + 1, :] for t in range(tiles)], axis=0)
    asked = jnp.concatenate([asked - tile * n_ocean, jnp.zeros((LANES - tiles, LANES), I32)], axis=0)
    asked = jnp.transpose(asked)
    where_col = lax.broadcasted_iota(I32, (nrows, n_ocean), 1)
    stacked = lax.rem(where_col, own) * per + lax.div(where_col, own)
    for t in range(tiles):
        hit = asked[0:nrows, t : t + 1] == stacked
        picks[t * nrows : (t + 1) * nrows, :] = jnp.where(hit, 1.0, 0.0).astype(BF16)

    gram_all = many(gram_recv, (tiles - 1) * 8, gram_ssem, gram_rsem)
    gram_all.wait_recv()
    total = jnp.sum(gram_recv[...].reshape(tiles, 8, LANES), axis=0)
    total = jnp.sum(total, axis=1, keepdims=True)
    n0, n1, n2, n3, n4, n5 = (total[k : k + 1, :] for k in range(6))

    def inverse(pivot, scale):
        good = pivot > 1e-6 * scale
        return jnp.where(good, 1.0 / jnp.where(good, pivot, 1.0), 0.0)

    i0 = inverse(n1, 0.0 * n1)
    l1, l2 = n2 * i0, n3 * i0
    d1, h = n3 - l1 * n2, n4 - l1 * n3
    i1 = inverse(d1, n3)
    l3 = h * i1
    d2 = n5 - l2 * n3 - l3 * h
    i2 = inverse(d2, n5)
    y1 = n1 - l1 * n0
    y2 = n2 - l2 * n0 - l3 * y1
    c2 = y2 * i2
    c1 = y1 * i1 - l3 * c2
    c0 = n0 * i0 - l1 * c1 - l2 * c2
    c0, c1, c2 = (jnp.broadcast_to(c, (1, LANES)) for c in (c0, c1, c2))

    loads["temp"].wait()
    for j in range(per):
        part = slice(j * LANES, (j + 1) * LANES)
        x = c0 * w0[j, HALO : HALO + own, :] + c1 * w1[j, HALO : HALO + own, :] + c2 * w2[j, HALO : HALO + own, :]
        height[:, part] = x
        sst[j * own : (j + 1) * own, :] = jnp.where(mask_ref[:, part] == 1, temp_ref[:, part] + x, 0.0).astype(BF16)

    rows_slot = pl.ds(pl.multiple_of(tile * nrows, nrows), nrows)
    wide_tiles = tiles // wide
    plane = lax.div(tile, wide_tiles)

    def rows_copy(other):
        return pltpu.make_async_remote_copy(
            src_ref=rows_send.at[pl.ds(pl.multiple_of(other * nrows, nrows), nrows)],
            dst_ref=rows_recv.at[rows_slot],
            send_sem=rows_ssem,
            recv_sem=rows_rsem,
            device_id=(group, other),
            device_id_type=MESH,
        )

    within = lax.rem(tile, wide_tiles)
    for dp in far_first(wide):
        goal = around(plane + dp, wide) * wide_tiles
        part = pl.ds(pl.multiple_of(goal * nrows, wide_tiles * nrows), wide_tiles * nrows)
        rows_send[part, :] = jnp.dot(picks[part, :], sst[...], preferred_element_type=F32).astype(BF16)
        for dt in far_first(wide_tiles):
            if dp or dt:
                rows_copy(goal + around(within + dt, wide_tiles)).start()
    rows_recv[rows_slot, :] = rows_send[rows_slot, :]
    rows_all = many(rows_recv, (tiles - 1) * nrows, rows_ssem, rows_rsem)
    rows_all.wait_recv()
    got = jnp.sum(rows_recv[...].astype(F32).reshape(tiles, nrows, LANES), axis=0)
    for k in range(nrows):
        rows_out[:, k * LANES : (k + 1) * LANES] = got[k : k + 1, :]

    requests.wait_send()
    many(flux_all, (n_chip - 1) * nrows, flux_ssem, flux_rsem.at[0]).wait_send()
    for g in range(groups):
        forward(g).wait_send()
    gram_all.wait_send()
    rows_all.wait_send()


def finish(pre, height, rows, column, atm_hbm, height_hbm, held, sems, height_sem):
    copy = pltpu.make_async_copy(height, height_hbm, height_sem)
    copy.start()
    lev, cols = pre.shape
    n_part = sems.shape[0]
    size = cols // n_part
    outs = []
    for i in range(n_part):
        part = pl.ds(i * size, size)
        for j in range(i * size, (i + 1) * size, LANES):
            held[:, j : j + LANES] = pre[:, j : j + LANES] + column[...] * rows[:, j : j + LANES]
        outs.append(pltpu.make_async_copy(held.at[:, part], atm_hbm.at[:, part], sems.at[i]))
        outs[-1].start()
    for out in outs:
        out.wait()
    copy.wait()


def solution(mesh):
    groups, tiles = mesh.shape["comp"], mesh.shape["tile"]
    count = groups * tiles

    def body(state, vco, weight, response, blocks, source, entry, present, mask, depth, temp, wanted):
        lev, cols = state.shape
        own, width = mask.shape
        nrows = cols // LANES
        n_flux = count * nrows
        n_ocean = own * width // LANES
        ext = own + 2 * HALO
        n_req = tiles * nrows
        n_chunk = max(1, cols // 1024)
        vmem = pl.BlockSpec(memory_space=pltpu.VMEM)
        n_block, n_entry = blocks.shape[0], source.shape[1]
        anywhere = pl.BlockSpec(memory_space=pltpu.HBM)
        dma = pltpu.SemaphoreType.DMA
        pre, height, rows, column = pl.pallas_call(
            functools.partial(kernel, groups, tiles),
            out_shape=(
                jax.ShapeDtypeStruct((lev, cols), F32),
                jax.ShapeDtypeStruct((own, width), F32),
                jax.ShapeDtypeStruct((1, cols), F32),
                jax.ShapeDtypeStruct((lev, LANES), F32),
            ),
            in_specs=[anywhere] * 12,
            out_specs=(vmem, vmem, vmem, vmem),
            scratch_shapes=[
                pltpu.VMEM((lev, cols), F32),
                pltpu.VMEM((lev, lev), F32),
                pltpu.VMEM((1, lev), F32),
                pltpu.VMEM((n_block, LANES, LANES), BF16),
                pltpu.VMEM((n_entry, n_ocean), I32),
                pltpu.VMEM((n_entry, n_ocean), I32),
                pltpu.VMEM((n_entry, n_ocean), I32),
                pltpu.VMEM((own, width), I32),
                pltpu.VMEM((own, width), F32),
                pltpu.VMEM((own, width), F32),
                pltpu.VMEM((1, nrows), I32),
                pltpu.VMEM((1, lev), F32),
                pltpu.VMEM((2 * lev, 2 * lev), BF16),
                pltpu.VMEM((nrows, LANES), F32),
                pltpu.VMEM((n_flux, LANES), BF16),
                pltpu.VMEM((n_block * n_flux + 8, LANES), F32),
                pltpu.VMEM((n_entry, 1, n_ocean + 2 * LANES), I32),
                pltpu.SMEM(((n_entry + 1) * (n_ocean + 2 * LANES),), I32),
                pltpu.VMEM((ext, width), F32),
                pltpu.VMEM((width // LANES, ext, LANES), F32),
                pltpu.VMEM((width // LANES, ext, LANES), F32),
                pltpu.VMEM((width // LANES, ext, LANES), F32),
                pltpu.VMEM((width // LANES, ext, LANES), F32),
                pltpu.VMEM((width // LANES, ext, LANES), F32),
                pltpu.VMEM((tiles * 8, LANES), I32),
                pltpu.VMEM((n_req, n_ocean), BF16),
                pltpu.VMEM((n_ocean, LANES), BF16),
                pltpu.VMEM((n_req, LANES), BF16),
                pltpu.VMEM((n_req, LANES), BF16),
                pltpu.VMEM((8, LANES), F32),
                pltpu.VMEM((tiles * 8, LANES), F32),
                dma((n_chunk,)),
                dma((11,)),
                dma((n_entry,)),
                dma,
                dma((groups,)),
                dma((groups,)),
                dma((groups,)),
                dma,
                dma,
                dma((4,)),
                dma((4,)),
                dma,
                dma,
                dma,
                dma,
            ],
            compiler_params=pltpu.CompilerParams(
                collective_id=0, has_side_effects=True, vmem_limit_bytes=48 * 1024 * 1024
            ),
        )(
            *(
                pltpu.with_memory_space_constraint(value, pltpu.HBM)
                for value in (
                    state,
                    vco,
                    weight[None, :],
                    blocks,
                    source.T,
                    entry.T,
                    present.T,
                    mask,
                    depth,
                    temp,
                    wanted[None, :],
                    response[None, :],
                )
            )
        )
        return pl.pallas_call(
            finish,
            out_shape=(jax.ShapeDtypeStruct((lev, cols), F32), jax.ShapeDtypeStruct((own, width), F32)),
            in_specs=[vmem] * 4,
            out_specs=(anywhere, anywhere),
            scratch_shapes=[pltpu.VMEM((lev, cols), F32), dma((n_chunk,)), dma],
            compiler_params=pltpu.CompilerParams(vmem_limit_bytes=16 * 1024 * 1024),
        )(pre, height, rows, column)

    split = P(None, ("comp", "tile"))
    ocean = P("tile", None)
    return jax.shard_map(
        body,
        mesh=mesh,
        in_specs=(split, P(), P(), P(), P(), ocean, ocean, ocean, ocean, ocean, ocean, P(("comp", "tile"))),
        out_specs=(split, ocean),
        check_vma=False,
    )
```

```python
import functools

import jax
import jax.numpy as jnp
from jax import lax
from jax.experimental import pallas as pl
from jax.experimental.pallas import tpu as pltpu
from jax.sharding import PartitionSpec as P

F32, BF16, I32 = jnp.float32, jnp.bfloat16, jnp.int32
MESH = pl.DeviceIdType.MESH
LANES = 128
HALO = 8
TIME_STEP = 0.5


FAR_FIRST = True


def hops(i, n):
    return min(i, n - i)


def kernel(
    groups,
    tiles,
    state_hbm,
    vco_hbm,
    weight_hbm,
    blocks_hbm,
    source_hbm,
    entry_hbm,
    present_hbm,
    mask_hbm,
    depth_hbm,
    temp_hbm,
    wanted_hbm,
    response_hbm,
    pre,
    height,
    rows_out,
    column_out,
    state,
    vco_ref,
    weight_ref,
    blocks_ref,
    source_ref,
    entry_ref,
    present_ref,
    mask_ref,
    depth_ref,
    temp_ref,
    wanted_ref,
    response_ref,
    vv,
    fluxf,
    flux_all,
    table,
    idx_v,
    idx_s,
    coef,
    inv,
    field,
    w0,
    w1,
    w2,
    req_v,
    picks,
    sst,
    rows_send,
    rows_recv,
    gram_send,
    gram_recv,
    in_sem,
    load_sem,
    idx_sem,
    flux_ssem,
    flux_rsem,
    fwd_ssem,
    fwd_rsem,
    req_ssem,
    req_rsem,
    halo_ssem,
    halo_rsem,
    gram_ssem,
    gram_rsem,
    rows_ssem,
    rows_rsem,
):
    group, tile = lax.axis_index("comp"), lax.axis_index("tile")
    count = groups * tiles
    lev, cols = state.shape
    own, width = mask_hbm.shape
    per = width // LANES
    ext = own + 2 * HALO
    nrows = cols // LANES
    n_flux = count * nrows
    n_entry, n_ocean = source_hbm.shape
    n_block = blocks_ref.shape[0]
    chunk = min(1024, cols)
    n_chunk = cols // chunk
    core, side = lax.rem(tile, 2), tiles // 2
    n_chip = groups * side
    partner = tile + 1 - 2 * core
    half = n_flux // 2
    part_rows = side * nrows
    span = n_ocean + 2 * LANES

    lane_of_chip = lax.div(tile, 2)
    chip = group * side + lane_of_chip

    def around(value, size):
        return jnp.where(value >= size, value - size, value)

    def far_first(n):
        return sorted(range(n), key=lambda i: -min(i, n - i))

    wide = 4 if side % 4 == 0 else 1
    chip_order = [a * (side // wide) + b for a in far_first(wide) for b in far_first(side // wide)]
    chip_order.sort(key=lambda q: -(hops(q // (side // wide), wide) + hops(q % (side // wide), side // wide)))
    order = far_first(groups) if FAR_FIRST else far_first(groups)[::-1]

    def chip_peer(dg, dq):
        return around(group + dg, groups), 2 * around(lane_of_chip + dq, side) + core

    def tile_peer(dt):
        return group, around(tile + dt, tiles)

    chip_offsets = [(dg, dq) for dg in order for dq in chip_order if dg or dq]
    tile_offsets = [2 * dq + dc for dq in chip_order for dc in (0, 1) if dq or dc]

    loads = {
        name: pltpu.make_async_copy(source, target, load_sem.at[i])
        for i, (name, source, target) in enumerate(
            (
                ("vco", vco_hbm, vco_ref),
                ("weight", weight_hbm, weight_ref),
                ("mask", mask_hbm, mask_ref),
                ("depth", depth_hbm, depth_ref),
                ("source", source_hbm, source_ref),
                ("entry", entry_hbm, entry_ref),
                ("present", present_hbm, present_ref),
                ("wanted", wanted_hbm, wanted_ref),
                ("blocks", blocks_hbm, blocks_ref),
                ("temp", temp_hbm, temp_ref),
                ("response", response_hbm, response_ref),
            )
        )
    }

    def load_state(i):
        part = pl.ds(i * chunk, chunk)
        return pltpu.make_async_copy(state_hbm.at[:, part], state.at[:, part], in_sem.at[i])

    barrier = pltpu.get_barrier_semaphore()
    greeted = [chip_peer(*d) for d in chip_offsets]
    greeted += [(group, 2 * around(lane_of_chip + dq, side) + 1 - core) for dq in chip_order]

    def greet(targets):
        for target in targets:
            pl.semaphore_signal(barrier, inc=1, device_id=target, device_id_type=MESH)

    loads["vco"].start()
    for i in range(n_chunk):
        load_state(i).start()
    greet(greeted)
    loads["weight"].start()
    for name in loads:
        if name not in ("vco", "weight"):
            loads[name].start()

    loads["vco"].wait()
    vco = vco_ref[...]
    v_hi = vco.astype(BF16)
    v_lo = (vco - v_hi.astype(F32)).astype(BF16)
    vv[0:lev, 0:lev] = v_hi
    vv[0:lev, lev : 2 * lev] = v_hi
    vv[lev : 2 * lev, 0:lev] = v_lo
    vv[lev : 2 * lev, lev : 2 * lev] = v_lo

    def tendency(s):
        hi = s.astype(BF16)
        lo = (s - hi.astype(F32)).astype(BF16)
        both = jnp.dot(vv[...], jnp.concatenate([hi, lo], axis=0), preferred_element_type=F32)
        return TIME_STEP * jnp.tanh(both[0:lev] + both[lev : 2 * lev])

    for i in range(n_chunk):
        load_state(i).wait()
    loads["weight"].wait()
    column = jnp.transpose(jnp.broadcast_to(weight_ref[...], (LANES, lev)))[:, 0:1]
    parts = [pl.ds(i * chunk, chunk) for i in range(n_chunk)]
    for part in parts:
        s = state[:, part]
        state[:, part] = s + tendency(s)
    for i, part in enumerate(parts):
        s = state[:, part]
        s = s + tendency(s)
        state[:, part] = s
        line = jnp.sum(s * column, axis=0, keepdims=True)
        for k in range(chunk // LANES):
            fluxf[i * (chunk // LANES) + k : i * (chunk // LANES) + k + 1, :] = line[:, k * LANES : (k + 1) * LANES]
    mine = pl.ds(pl.multiple_of(core * half + chip * nrows, nrows), nrows)
    flux_all[mine, :] = fluxf[...].astype(BF16)

    for name in ("source", "entry", "present"):
        loads[name].wait()
    spare = n_block * n_flux
    source = source_ref[...]
    holder = lax.div(source, nrows)
    row = lax.rem(holder, 2) * half + lax.div(holder, 2) * nrows + lax.rem(source, nrows)
    index = jnp.where(present_ref[...] == 1, entry_ref[...] * n_flux + row, jnp.full(source.shape, spare, I32))
    for k in range(n_entry):
        idx_v[k, :, LANES : LANES + n_ocean] = index[k : k + 1, :]
    table[pl.ds(spare, 8), :] = jnp.zeros((8, LANES), F32)

    pl.semaphore_wait(barrier, n_chip - 1 + side)

    def many(ref, rows, send_sem, recv_sem):
        return pltpu.make_async_remote_copy(
            src_ref=ref.at[pl.ds(0, rows)],
            dst_ref=ref.at[pl.ds(0, rows)],
            send_sem=send_sem,
            recv_sem=recv_sem,
            device_id=(group, partner),
            device_id_type=MESH,
        )

    after, before = lax.rem(tile + 1, tiles), lax.rem(tile + tiles - 1, tiles)

    def halo(ref, src, dst, k, target):
        return pltpu.make_async_remote_copy(
            src_ref=ref.at[src],
            dst_ref=ref.at[dst],
            send_sem=halo_ssem.at[k],
            recv_sem=halo_rsem.at[k],
            device_id=(group, target),
            device_id_type=MESH,
        )

    everything = slice(None)
    halos = (
        halo(coef, (pl.ds(own, HALO), everything), (pl.ds(0, HALO), everything), 0, after),
        halo(coef, (pl.ds(HALO, HALO), everything), (pl.ds(HALO + own, HALO), everything), 1, before),
        halo(idx_v, (everything, everything, pl.ds(n_ocean, LANES)), (everything, everything, pl.ds(0, LANES)), 2, after),
        halo(
            idx_v,
            (everything, everything, pl.ds(LANES, LANES)),
            (everything, everything, pl.ds(LANES + n_ocean, LANES)),
            3,
            before,
        ),
    )
    for copy in halos[2:]:
        copy.start()

    def flux_copy(target):
        return pltpu.make_async_remote_copy(
            src_ref=flux_all.at[mine],
            dst_ref=flux_all.at[mine],
            send_sem=flux_ssem,
            recv_sem=flux_rsem.at[group],
            device_id=target,
            device_id_type=MESH,
        )

    for d in chip_offsets:
        flux_copy(chip_peer(*d)).start()

    for name in ("mask", "depth", "wanted"):
        loads[name].wait()
    coef[HALO : HALO + own, :] = mask_ref[...].astype(F32) * (4.0 + depth_ref[...])
    own_slot = pl.ds(pl.multiple_of(tile * 8, 8), 8)
    req_v[own_slot, :] = jnp.full((8, LANES), -1, I32)
    req_v[own_slot, 0:nrows] = jnp.broadcast_to(wanted_ref[...], (8, nrows))

    def request(target):
        return pltpu.make_async_remote_copy(
            src_ref=req_v.at[own_slot],
            dst_ref=req_v.at[own_slot],
            send_sem=req_ssem,
            recv_sem=req_rsem,
            device_id=target,
            device_id_type=MESH,
        )

    for d in tile_offsets:
        request(tile_peer(d)).start()
    requests = many(req_v, (tiles - 1) * 8, req_ssem, req_rsem)

    for copy in halos[:2]:
        copy.start()

    for i in range(n_chunk):
        part = pl.ds(i * chunk, chunk)
        s = state[:, part]
        pre[:, part] = s + tendency(s)

    loads["response"].wait()
    column_out[...] = TIME_STEP * jnp.transpose(jnp.broadcast_to(response_ref[...], (LANES, lev)))

    zero_rows = jnp.zeros((per, HALO, LANES), F32)
    field[:, 0:HALO, :] = zero_rows
    field[:, HALO + own : ext, :] = zero_rows

    def reciprocal(value):
        return jnp.where(value > 0.0, 1.0 / jnp.where(value > 0.0, value, 1.0), 0.0)

    def set_inverse(first, last, exists):
        for j in range(per):
            value = reciprocal(coef[first:last, j * LANES : (j + 1) * LANES])
            inv[j, first:last, :] = value if exists is None else jnp.where(exists, value, 0.0)

    set_inverse(HALO, HALO + own, None)

    loads["blocks"].wait()
    pairs = [jnp.concatenate([blocks_ref[b], blocks_ref[b + 1]], axis=1) for b in range(0, n_block, 2)]

    def products(at):
        some = flux_all[pl.ds(pl.multiple_of(at, part_rows), part_rows), :]
        for b, pair in enumerate(pairs):
            got = jnp.dot(some, pair, preferred_element_type=F32)
            for k in range(2):
                to = pl.multiple_of((2 * b + k) * n_flux + at, part_rows)
                table[pl.ds(to, part_rows), :] = got[:, k * LANES : (k + 1) * LANES]

    def forward(g):
        slot = pl.ds(pl.multiple_of(core * half + g * part_rows, part_rows), part_rows)
        return pltpu.make_async_remote_copy(
            src_ref=flux_all.at[slot],
            dst_ref=flux_all.at[slot],
            send_sem=fwd_ssem.at[g],
            recv_sem=fwd_rsem.at[g],
            device_id=(group, partner),
            device_id_type=MESH,
        )

    def take(offset):
        g = around(group + offset, groups)
        blocks_in = side - 1 if offset == 0 else side
        many(flux_all, blocks_in * nrows, flux_ssem, flux_rsem.at[g]).wait_recv()
        forward(g).start()

    def near(offset):
        products(core * half + around(group + offset, groups) * part_rows)

    def far(offset):
        products((1 - core) * half + around(group + offset, groups) * part_rows)

    def shared(offset):
        forward(around(group + offset, groups)).wait_recv()

    ahead, behind = order[: len(order) // 2], order[len(order) // 2 :]

    @pl.when(core == 1)
    def _():
        for offset in ahead:
            take(offset)
            near(offset)
        for offset in behind:
            take(offset)
        for offset in behind:
            near(offset)

    @pl.when(core == 0)
    def _():
        for offset in ahead:
            shared(offset)
            far(offset)
        for offset in ahead:
            take(offset)
        for offset in ahead:
            near(offset)
        for offset in behind:
            take(offset)

    for copy in halos[2:]:
        copy.wait()
    index_copies = [
        pltpu.make_async_copy(idx_v.at[k, 0], idx_s.at[pl.ds(k * span, span)], idx_sem.at[k]) for k in range(n_entry)
    ]
    for copy in index_copies:
        copy.start()

    @pl.when(core == 1)
    def _():
        for some in (ahead, behind):
            for offset in some:
                shared(offset)
            for offset in some:
                far(offset)

    @pl.when(core == 0)
    def _():
        for offset in behind:
            shared(offset)
        for offset in behind:
            far(offset)
            near(offset)

    def forcing_rows(g_tile, j, rows):
        first_row = g_tile * 8 * per + j + (rows[0] - HALO) * per + LANES
        totals = []
        for s in rows:
            e = first_row + (s - rows[0]) * per
            got = [table[pl.ds(idx_s.at[pl.ds(e + k * span, 1)][0], 1), :] for k in range(n_entry)]
            while len(got) > 1:
                got = [sum(got[k : k + 2][1:], got[k]) for k in range(0, len(got), 2)]
            totals.append(got[0])
        at = pl.multiple_of(g_tile * 8, 8)
        block = field.at[j, pl.ds(at, 8), :]
        for s, total in zip(rows, totals):
            block[s : s + 1, :] = total

    def edge(j, carry):
        forcing_rows(0, j, (HALO - 3, HALO - 2, HALO - 1))
        forcing_rows(ext // 8 - 1, j, (0, 1, 2))
        return carry

    for copy in index_copies:
        copy.wait()
    lax.fori_loop(0, per, edge, 0)

    def inside_rows(g_tile, carry):
        def one(j, inner):
            forcing_rows(g_tile, j, range(8))
            return inner

        return lax.fori_loop(0, per, one, carry, unroll=5)

    lax.fori_loop(1, 1 + own // 8, inside_rows, 0)

    for copy in halos[:2]:
        copy.wait()
    set_inverse(0, HALO, tile > 0)
    set_inverse(HALO + own, ext, tile < tiles - 1)

    n_tile = ext // 8
    lane = lax.broadcasted_iota(I32, (per, 8, LANES), 2)

    def rows8(ref, k):
        return ref[:, 8 * k : 8 * k + 8, :]

    def beside(ref, k):
        here = rows8(ref, k)
        up = ref[:, 8 * k - 1 : 8 * k + 7, :] if k > 0 else pltpu.roll(here, 1, 1)
        down = ref[:, 8 * k + 1 : 8 * k + 9, :] if k < n_tile - 1 else pltpu.roll(here, 7, 1)
        one, other = pltpu.roll(here, 1, 2), pltpu.roll(here, LANES - 1, 2)
        left = jnp.where(lane == 0, jnp.concatenate([one[per - 1 :], one[: per - 1]], axis=0), one)
        right = jnp.where(lane == LANES - 1, jnp.concatenate([other[1:], other[:1]], axis=0), other)
        return (up + down) + (left + right)

    nothing = jnp.zeros((8, LANES), F32)
    own_tiles = range(1, n_tile - 1)

    nu0 = nothing
    for k in range(n_tile):
        f = rows8(field, k)
        w = rows8(inv, k) * f
        w0[:, 8 * k : 8 * k + 8, :] = w
        if k in own_tiles:
            nu0 = nu0 + jnp.sum(w * f, axis=0)

    def apply(w_old, w_new):
        a, b = nothing, nothing
        for k in range(n_tile):
            q = rows8(field, k) - beside(w_old, k)
            w = rows8(inv, k) * q
            field[:, 8 * k : 8 * k + 8, :] = q
            w_new[:, 8 * k : 8 * k + 8, :] = w
            if k in own_tiles:
                a = a + jnp.sum(rows8(w_old, k) * q, axis=0)
                b = b + jnp.sum(w * q, axis=0)
        return a, b

    nu1, nu2 = apply(w0, w1)
    nu3, nu4 = apply(w1, w2)
    nu5 = nothing
    for k in own_tiles:
        nu5 = nu5 + jnp.sum(rows8(w2, k) * (rows8(field, k) - beside(w2, k)), axis=0)

    gram_send[...] = jnp.zeros((8, LANES), F32)
    for k, nu in enumerate((nu0, nu1, nu2, nu3, nu4, nu5)):
        gram_send[k : k + 1, :] = jnp.sum(nu, axis=0, keepdims=True)
    gram_slot = pl.ds(pl.multiple_of(tile * 8, 8), 8)
    gram_recv[gram_slot, :] = gram_send[...]

    def gram_copy(target):
        return pltpu.make_async_remote_copy(
            src_ref=gram_send,
            dst_ref=gram_recv.at[gram_slot],
            send_sem=gram_ssem,
            recv_sem=gram_rsem,
            device_id=target,
            device_id_type=MESH,
        )

    for d in tile_offsets:
        gram_copy(tile_peer(d)).start()
    requests.wait_recv()
    asked = jnp.concatenate([req_v[8 * t : 8 * t + 1, :] for t in range(tiles)], axis=0)
    asked = jnp.concatenate([asked - tile * n_ocean, jnp.zeros((LANES - tiles, LANES), I32)], axis=0)
    asked = jnp.transpose(asked)
    where_col = lax.broadcasted_iota(I32, (nrows, n_ocean), 1)
    stacked = lax.rem(where_col, own) * per + lax.div(where_col, own)
    for t in range(tiles):
        hit = asked[0:nrows, t : t + 1] == stacked
        picks[t * nrows : (t + 1) * nrows, :] = jnp.where(hit, 1.0, 0.0).astype(BF16)

    gram_all = many(gram_recv, (tiles - 1) * 8, gram_ssem, gram_rsem)
    gram_all.wait_recv()
    total = jnp.sum(gram_recv[...].reshape(tiles, 8, LANES), axis=0)
    total = jnp.sum(total, axis=1, keepdims=True)
    n0, n1, n2, n3, n4, n5 = (total[k : k + 1, :] for k in range(6))

    def inverse(pivot, scale):
        good = pivot > 1e-6 * scale
        return jnp.where(good, 1.0 / jnp.where(good, pivot, 1.0), 0.0)

    i0 = inverse(n1, 0.0 * n1)
    l1, l2 = n2 * i0, n3 * i0
    d1, h = n3 - l1 * n2, n4 - l1 * n3
    i1 = inverse(d1, n3)
    l3 = h * i1
    d2 = n5 - l2 * n3 - l3 * h
    i2 = inverse(d2, n5)
    y1 = n1 - l1 * n0
    y2 = n2 - l2 * n0 - l3 * y1
    c2 = y2 * i2
    c1 = y1 * i1 - l3 * c2
    c0 = n0 * i0 - l1 * c1 - l2 * c2
    c0, c1, c2 = (jnp.broadcast_to(c, (1, LANES)) for c in (c0, c1, c2))

    loads["temp"].wait()
    for j in range(per):
        part = slice(j * LANES, (j + 1) * LANES)
        x = c0 * w0[j, HALO : HALO + own, :] + c1 * w1[j, HALO : HALO + own, :] + c2 * w2[j, HALO : HALO + own, :]
        height[:, part] = x
        sst[j * own : (j + 1) * own, :] = jnp.where(mask_ref[:, part] == 1, temp_ref[:, part] + x, 0.0).astype(BF16)

    rows_slot = pl.ds(pl.multiple_of(tile * nrows, nrows), nrows)
    wide_tiles = tiles // wide
    plane = lax.div(tile, wide_tiles)

    def rows_copy(other):
        return pltpu.make_async_remote_copy(
            src_ref=rows_send.at[pl.ds(pl.multiple_of(other * nrows, nrows), nrows)],
            dst_ref=rows_recv.at[rows_slot],
            send_sem=rows_ssem,
            recv_sem=rows_rsem,
            device_id=(group, other),
            device_id_type=MESH,
        )

    within = lax.rem(tile, wide_tiles)
    for dp in far_first(wide):
        goal = around(plane + dp, wide) * wide_tiles
        part = pl.ds(pl.multiple_of(goal * nrows, wide_tiles * nrows), wide_tiles * nrows)
        rows_send[part, :] = jnp.dot(picks[part, :], sst[...], preferred_element_type=F32).astype(BF16)
        for dt in far_first(wide_tiles):
            if dp or dt:
                rows_copy(goal + around(within + dt, wide_tiles)).start()
    rows_recv[rows_slot, :] = rows_send[rows_slot, :]
    rows_all = many(rows_recv, (tiles - 1) * nrows, rows_ssem, rows_rsem)
    rows_all.wait_recv()
    got = jnp.sum(rows_recv[...].astype(F32).reshape(tiles, nrows, LANES), axis=0)
    for k in range(nrows):
        rows_out[:, k * LANES : (k + 1) * LANES] = got[k : k + 1, :]

    requests.wait_send()
    many(flux_all, (n_chip - 1) * nrows, flux_ssem, flux_rsem.at[0]).wait_send()
    for g in range(groups):
        forward(g).wait_send()
    gram_all.wait_send()
    rows_all.wait_send()


def finish(pre, height, rows, column, atm_hbm, height_hbm, held, sems, height_sem):
    copy = pltpu.make_async_copy(height, height_hbm, height_sem)
    copy.start()
    lev, cols = pre.shape
    n_part = sems.shape[0]
    size = cols // n_part
    outs = []
    for i in range(n_part):
        part = pl.ds(i * size, size)
        for j in range(i * size, (i + 1) * size, LANES):
            held[:, j : j + LANES] = pre[:, j : j + LANES] + column[...] * rows[:, j : j + LANES]
        outs.append(pltpu.make_async_copy(held.at[:, part], atm_hbm.at[:, part], sems.at[i]))
        outs[-1].start()
    for out in outs:
        out.wait()
    copy.wait()


def solution(mesh):
    groups, tiles = mesh.shape["comp"], mesh.shape["tile"]
    count = groups * tiles

    def body(state, vco, weight, response, blocks, source, entry, present, mask, depth, temp, wanted):
        lev, cols = state.shape
        own, width = mask.shape
        nrows = cols // LANES
        n_flux = count * nrows
        n_ocean = own * width // LANES
        ext = own + 2 * HALO
        n_req = tiles * nrows
        n_chunk = max(1, cols // 1024)
        vmem = pl.BlockSpec(memory_space=pltpu.VMEM)
        n_block, n_entry = blocks.shape[0], source.shape[1]
        anywhere = pl.BlockSpec(memory_space=pltpu.HBM)
        dma = pltpu.SemaphoreType.DMA
        pre, height, rows, column = pl.pallas_call(
            functools.partial(kernel, groups, tiles),
            out_shape=(
                jax.ShapeDtypeStruct((lev, cols), F32),
                jax.ShapeDtypeStruct((own, width), F32),
                jax.ShapeDtypeStruct((1, cols), F32),
                jax.ShapeDtypeStruct((lev, LANES), F32),
            ),
            in_specs=[anywhere] * 12,
            out_specs=(vmem, vmem, vmem, vmem),
            scratch_shapes=[
                pltpu.VMEM((lev, cols), F32),
                pltpu.VMEM((lev, lev), F32),
                pltpu.VMEM((1, lev), F32),
                pltpu.VMEM((n_block, LANES, LANES), BF16),
                pltpu.VMEM((n_entry, n_ocean), I32),
                pltpu.VMEM((n_entry, n_ocean), I32),
                pltpu.VMEM((n_entry, n_ocean), I32),
                pltpu.VMEM((own, width), I32),
                pltpu.VMEM((own, width), F32),
                pltpu.VMEM((own, width), F32),
                pltpu.VMEM((1, nrows), I32),
                pltpu.VMEM((1, lev), F32),
                pltpu.VMEM((2 * lev, 2 * lev), BF16),
                pltpu.VMEM((nrows, LANES), F32),
                pltpu.VMEM((n_flux, LANES), BF16),
                pltpu.VMEM((n_block * n_flux + 8, LANES), F32),
                pltpu.VMEM((n_entry, 1, n_ocean + 2 * LANES), I32),
                pltpu.SMEM(((n_entry + 1) * (n_ocean + 2 * LANES),), I32),
                pltpu.VMEM((ext, width), F32),
                pltpu.VMEM((width // LANES, ext, LANES), F32),
                pltpu.VMEM((width // LANES, ext, LANES), F32),
                pltpu.VMEM((width // LANES, ext, LANES), F32),
                pltpu.VMEM((width // LANES, ext, LANES), F32),
                pltpu.VMEM((width // LANES, ext, LANES), F32),
                pltpu.VMEM((tiles * 8, LANES), I32),
                pltpu.VMEM((n_req, n_ocean), BF16),
                pltpu.VMEM((n_ocean, LANES), BF16),
                pltpu.VMEM((n_req, LANES), BF16),
                pltpu.VMEM((n_req, LANES), BF16),
                pltpu.VMEM((8, LANES), F32),
                pltpu.VMEM((tiles * 8, LANES), F32),
                dma((n_chunk,)),
                dma((11,)),
                dma((n_entry,)),
                dma,
                dma((groups,)),
                dma((groups,)),
                dma((groups,)),
                dma,
                dma,
                dma((4,)),
                dma((4,)),
                dma,
                dma,
                dma,
                dma,
            ],
            compiler_params=pltpu.CompilerParams(
                collective_id=0, has_side_effects=True, vmem_limit_bytes=48 * 1024 * 1024
            ),
        )(
            *(
                pltpu.with_memory_space_constraint(value, pltpu.HBM)
                for value in (
                    state,
                    vco,
                    weight[None, :],
                    blocks,
                    source.T,
                    entry.T,
                    present.T,
                    mask,
                    depth,
                    temp,
                    wanted[None, :],
                    response[None, :],
                )
            )
        )
        return pl.pallas_call(
            finish,
            out_shape=(jax.ShapeDtypeStruct((lev, cols), F32), jax.ShapeDtypeStruct((own, width), F32)),
            in_specs=[vmem] * 4,
            out_specs=(anywhere, anywhere),
            scratch_shapes=[pltpu.VMEM((lev, cols), F32), dma((n_chunk,)), dma],
            compiler_params=pltpu.CompilerParams(vmem_limit_bytes=16 * 1024 * 1024),
        )(pre, height, rows, column)

    split = P(None, ("comp", "tile"))
    ocean = P("tile", None)
    return jax.shard_map(
        body,
        mesh=mesh,
        in_specs=(split, P(), P(), P(), P(), ocean, ocean, ocean, ocean, ocean, ocean, P(("comp", "tile"))),
        out_specs=(split, ocean),
        check_vma=False,
    )
```

```python
import functools

import jax
import jax.numpy as jnp
from jax import lax
from jax.experimental import pallas as pl
from jax.experimental.pallas import tpu as pltpu
from jax.sharding import PartitionSpec as P

F32, BF16, I32 = jnp.float32, jnp.bfloat16, jnp.int32
MESH = pl.DeviceIdType.MESH
LANES = 128
HALO = 8
TIME_STEP = 0.5


FAR_FIRST = True


def hops(i, n):
    return min(i, n - i)


def kernel(
    groups,
    tiles,
    state_hbm,
    vco_hbm,
    weight_hbm,
    blocks_hbm,
    source_hbm,
    entry_hbm,
    present_hbm,
    mask_hbm,
    depth_hbm,
    temp_hbm,
    wanted_hbm,
    response_hbm,
    pre,
    height,
    rows_out,
    column_out,
    state,
    vco_ref,
    weight_ref,
    blocks_ref,
    source_ref,
    entry_ref,
    present_ref,
    mask_ref,
    depth_ref,
    temp_ref,
    wanted_ref,
    response_ref,
    vv,
    fluxf,
    flux_all,
    table,
    idx_v,
    idx_s,
    coef,
    inv,
    field,
    w0,
    w1,
    w2,
    req_v,
    picks,
    sst,
    rows_send,
    rows_recv,
    gram_send,
    gram_recv,
    in_sem,
    load_sem,
    idx_sem,
    flux_ssem,
    flux_rsem,
    fwd_ssem,
    fwd_rsem,
    req_ssem,
    req_rsem,
    halo_ssem,
    halo_rsem,
    gram_ssem,
    gram_rsem,
    rows_ssem,
    rows_rsem,
):
    group, tile = lax.axis_index("comp"), lax.axis_index("tile")
    count = groups * tiles
    lev, cols = state.shape
    own, width = mask_hbm.shape
    per = width // LANES
    ext = own + 2 * HALO
    nrows = cols // LANES
    n_flux = count * nrows
    n_entry, n_ocean = source_hbm.shape
    n_block = blocks_ref.shape[0]
    chunk = min(1024, cols)
    n_chunk = cols // chunk
    core, side = lax.rem(tile, 2), tiles // 2
    n_chip = groups * side
    partner = tile + 1 - 2 * core
    half = n_flux // 2
    part_rows = side * nrows
    span = n_ocean + 2 * LANES

    lane_of_chip = lax.div(tile, 2)
    chip = group * side + lane_of_chip

    def around(value, size):
        return jnp.where(value >= size, value - size, value)

    def far_first(n):
        return sorted(range(n), key=lambda i: -min(i, n - i))

    wide = 4 if side % 4 == 0 else 1
    chip_order = [a * (side // wide) + b for a in far_first(wide) for b in far_first(side // wide)]
    chip_order.sort(key=lambda q: -(hops(q // (side // wide), wide) + hops(q % (side // wide), side // wide)))
    order = far_first(groups) if FAR_FIRST else far_first(groups)[::-1]

    def chip_peer(dg, dq):
        return around(group + dg, groups), 2 * around(lane_of_chip + dq, side) + core

    def tile_peer(dt):
        return group, around(tile + dt, tiles)

    chip_offsets = [(dg, dq) for dg in order for dq in chip_order if dg or dq]
    across = side // wide

    def distance(offset):
        dg, dq = offset
        return hops(dg, groups) + hops(dq // across, wide) + hops(dq % across, across)

    chip_offsets.sort(key=lambda offset: -distance(offset))
    tile_offsets = [2 * dq + dc for dq in chip_order for dc in (0, 1) if dq or dc]

    loads = {
        name: pltpu.make_async_copy(source, target, load_sem.at[i])
        for i, (name, source, target) in enumerate(
            (
                ("vco", vco_hbm, vco_ref),
                ("weight", weight_hbm, weight_ref),
                ("mask", mask_hbm, mask_ref),
                ("depth", depth_hbm, depth_ref),
                ("source", source_hbm, source_ref),
                ("entry", entry_hbm, entry_ref),
                ("present", present_hbm, present_ref),
                ("wanted", wanted_hbm, wanted_ref),
                ("blocks", blocks_hbm, blocks_ref),
                ("temp", temp_hbm, temp_ref),
                ("response", response_hbm, response_ref),
            )
        )
    }

    def load_state(i):
        part = pl.ds(i * chunk, chunk)
        return pltpu.make_async_copy(state_hbm.at[:, part], state.at[:, part], in_sem.at[i])

    barrier = pltpu.get_barrier_semaphore()
    greeted = [chip_peer(*d) for d in chip_offsets]
    greeted += [(group, 2 * around(lane_of_chip + dq, side) + 1 - core) for dq in chip_order]

    def greet(targets):
        for target in targets:
            pl.semaphore_signal(barrier, inc=1, device_id=target, device_id_type=MESH)

    loads["vco"].start()
    for i in range(n_chunk):
        load_state(i).start()
    greet(greeted)
    loads["weight"].start()
    for name in loads:
        if name not in ("vco", "weight"):
            loads[name].start()

    loads["vco"].wait()
    vco = vco_ref[...]
    v_hi = vco.astype(BF16)
    v_lo = (vco - v_hi.astype(F32)).astype(BF16)
    vv[0:lev, 0:lev] = v_hi
    vv[0:lev, lev : 2 * lev] = v_hi
    vv[lev : 2 * lev, 0:lev] = v_lo
    vv[lev : 2 * lev, lev : 2 * lev] = v_lo

    def tendency(s):
        hi = s.astype(BF16)
        lo = (s - hi.astype(F32)).astype(BF16)
        both = jnp.dot(vv[...], jnp.concatenate([hi, lo], axis=0), preferred_element_type=F32)
        return TIME_STEP * jnp.tanh(both[0:lev] + both[lev : 2 * lev])

    for i in range(n_chunk):
        load_state(i).wait()
    loads["weight"].wait()
    column = jnp.transpose(jnp.broadcast_to(weight_ref[...], (LANES, lev)))[:, 0:1]
    parts = [pl.ds(i * chunk, chunk) for i in range(n_chunk)]
    for part in parts:
        s = state[:, part]
        state[:, part] = s + tendency(s)
    for i, part in enumerate(parts):
        s = state[:, part]
        s = s + tendency(s)
        state[:, part] = s
        line = jnp.sum(s * column, axis=0, keepdims=True)
        for k in range(chunk // LANES):
            fluxf[i * (chunk // LANES) + k : i * (chunk // LANES) + k + 1, :] = line[:, k * LANES : (k + 1) * LANES]
    mine = pl.ds(pl.multiple_of(core * half + chip * nrows, nrows), nrows)
    flux_all[mine, :] = fluxf[...].astype(BF16)

    for name in ("source", "entry", "present"):
        loads[name].wait()
    spare = n_block * n_flux
    source = source_ref[...]
    holder = lax.div(source, nrows)
    row = lax.rem(holder, 2) * half + lax.div(holder, 2) * nrows + lax.rem(source, nrows)
    index = jnp.where(present_ref[...] == 1, entry_ref[...] * n_flux + row, jnp.full(source.shape, spare, I32))
    for k in range(n_entry):
        idx_v[k, :, LANES : LANES + n_ocean] = index[k : k + 1, :]
    table[pl.ds(spare, 8), :] = jnp.zeros((8, LANES), F32)

    pl.semaphore_wait(barrier, n_chip - 1 + side)

    def many(ref, rows, send_sem, recv_sem):
        return pltpu.make_async_remote_copy(
            src_ref=ref.at[pl.ds(0, rows)],
            dst_ref=ref.at[pl.ds(0, rows)],
            send_sem=send_sem,
            recv_sem=recv_sem,
            device_id=(group, partner),
            device_id_type=MESH,
        )

    after, before = lax.rem(tile + 1, tiles), lax.rem(tile + tiles - 1, tiles)

    def halo(ref, src, dst, k, target):
        return pltpu.make_async_remote_copy(
            src_ref=ref.at[src],
            dst_ref=ref.at[dst],
            send_sem=halo_ssem.at[k],
            recv_sem=halo_rsem.at[k],
            device_id=(group, target),
            device_id_type=MESH,
        )

    everything = slice(None)
    halos = (
        halo(coef, (pl.ds(own, HALO), everything), (pl.ds(0, HALO), everything), 0, after),
        halo(coef, (pl.ds(HALO, HALO), everything), (pl.ds(HALO + own, HALO), everything), 1, before),
        halo(idx_v, (everything, everything, pl.ds(n_ocean, LANES)), (everything, everything, pl.ds(0, LANES)), 2, after),
        halo(
            idx_v,
            (everything, everything, pl.ds(LANES, LANES)),
            (everything, everything, pl.ds(LANES + n_ocean, LANES)),
            3,
            before,
        ),
    )
    for copy in halos[2:]:
        copy.start()

    def flux_copy(target):
        return pltpu.make_async_remote_copy(
            src_ref=flux_all.at[mine],
            dst_ref=flux_all.at[mine],
            send_sem=flux_ssem,
            recv_sem=flux_rsem.at[group],
            device_id=target,
            device_id_type=MESH,
        )

    for d in chip_offsets:
        flux_copy(chip_peer(*d)).start()

    for name in ("mask", "depth", "wanted"):
        loads[name].wait()
    coef[HALO : HALO + own, :] = mask_ref[...].astype(F32) * (4.0 + depth_ref[...])
    own_slot = pl.ds(pl.multiple_of(tile * 8, 8), 8)
    req_v[own_slot, :] = jnp.full((8, LANES), -1, I32)
    req_v[own_slot, 0:nrows] = jnp.broadcast_to(wanted_ref[...], (8, nrows))

    def request(target):
        return pltpu.make_async_remote_copy(
            src_ref=req_v.at[own_slot],
            dst_ref=req_v.at[own_slot],
            send_sem=req_ssem,
            recv_sem=req_rsem,
            device_id=target,
            device_id_type=MESH,
        )

    for d in tile_offsets:
        request(tile_peer(d)).start()
    requests = many(req_v, (tiles - 1) * 8, req_ssem, req_rsem)

    for copy in halos[:2]:
        copy.start()

    for i in range(n_chunk):
        part = pl.ds(i * chunk, chunk)
        s = state[:, part]
        pre[:, part] = s + tendency(s)

    loads["response"].wait()
    column_out[...] = TIME_STEP * jnp.transpose(jnp.broadcast_to(response_ref[...], (LANES, lev)))

    zero_rows = jnp.zeros((per, HALO, LANES), F32)
    field[:, 0:HALO, :] = zero_rows
    field[:, HALO + own : ext, :] = zero_rows

    def reciprocal(value):
        return jnp.where(value > 0.0, 1.0 / jnp.where(value > 0.0, value, 1.0), 0.0)

    def set_inverse(first, last, exists):
        for j in range(per):
            value = reciprocal(coef[first:last, j * LANES : (j + 1) * LANES])
            inv[j, first:last, :] = value if exists is None else jnp.where(exists, value, 0.0)

    set_inverse(HALO, HALO + own, None)

    loads["blocks"].wait()
    pairs = [jnp.concatenate([blocks_ref[b], blocks_ref[b + 1]], axis=1) for b in range(0, n_block, 2)]

    def products(at):
        some = flux_all[pl.ds(pl.multiple_of(at, part_rows), part_rows), :]
        for b, pair in enumerate(pairs):
            got = jnp.dot(some, pair, preferred_element_type=F32)
            for k in range(2):
                to = pl.multiple_of((2 * b + k) * n_flux + at, part_rows)
                table[pl.ds(to, part_rows), :] = got[:, k * LANES : (k + 1) * LANES]

    def forward(g):
        slot = pl.ds(pl.multiple_of(core * half + g * part_rows, part_rows), part_rows)
        return pltpu.make_async_remote_copy(
            src_ref=flux_all.at[slot],
            dst_ref=flux_all.at[slot],
            send_sem=fwd_ssem.at[g],
            recv_sem=fwd_rsem.at[g],
            device_id=(group, partner),
            device_id_type=MESH,
        )

    def take(offset):
        g = around(group + offset, groups)
        blocks_in = side - 1 if offset == 0 else side
        many(flux_all, blocks_in * nrows, flux_ssem, flux_rsem.at[g]).wait_recv()
        forward(g).start()

    def near(offset):
        products(core * half + around(group + offset, groups) * part_rows)

    def far(offset):
        products((1 - core) * half + around(group + offset, groups) * part_rows)

    def shared(offset):
        forward(around(group + offset, groups)).wait_recv()

    ahead, behind = order[: len(order) // 2], order[len(order) // 2 :]

    @pl.when(core == 1)
    def _():
        for offset in ahead:
            take(offset)
            near(offset)
        for offset in behind:
            take(offset)
        for offset in behind:
            near(offset)

    @pl.when(core == 0)
    def _():
        for offset in ahead:
            shared(offset)
            far(offset)
        for offset in ahead:
            take(offset)
        for offset in ahead:
            near(offset)
        for offset in behind:
            take(offset)

    for copy in halos[2:]:
        copy.wait()
    index_copies = [
        pltpu.make_async_copy(idx_v.at[k, 0], idx_s.at[pl.ds(k * span, span)], idx_sem.at[k]) for k in range(n_entry)
    ]
    for copy in index_copies:
        copy.start()

    @pl.when(core == 1)
    def _():
        for some in (ahead, behind):
            for offset in some:
                shared(offset)
            for offset in some:
                far(offset)

    @pl.when(core == 0)
    def _():
        for offset in behind:
            shared(offset)
        for offset in behind:
            far(offset)
            near(offset)

    def forcing_rows(g_tile, j, rows):
        first_row = g_tile * 8 * per + j + (rows[0] - HALO) * per + LANES
        totals = []
        for s in rows:
            e = first_row + (s - rows[0]) * per
            got = [table[pl.ds(idx_s.at[pl.ds(e + k * span, 1)][0], 1), :] for k in range(n_entry)]
            while len(got) > 1:
                got = [sum(got[k : k + 2][1:], got[k]) for k in range(0, len(got), 2)]
            totals.append(got[0])
        at = pl.multiple_of(g_tile * 8, 8)
        block = field.at[j, pl.ds(at, 8), :]
        for s, total in zip(rows, totals):
            block[s : s + 1, :] = total

    def edge(j, carry):
        forcing_rows(0, j, (HALO - 3, HALO - 2, HALO - 1))
        forcing_rows(ext // 8 - 1, j, (0, 1, 2))
        return carry

    for copy in index_copies:
        copy.wait()
    lax.fori_loop(0, per, edge, 0)

    def inside_rows(g_tile, carry):
        def one(j, inner):
            forcing_rows(g_tile, j, range(8))
            return inner

        return lax.fori_loop(0, per, one, carry, unroll=5)

    lax.fori_loop(1, 1 + own // 8, inside_rows, 0)

    for copy in halos[:2]:
        copy.wait()
    set_inverse(0, HALO, tile > 0)
    set_inverse(HALO + own, ext, tile < tiles - 1)

    n_tile = ext // 8
    lane = lax.broadcasted_iota(I32, (per, 8, LANES), 2)

    def rows8(ref, k):
        return ref[:, 8 * k : 8 * k + 8, :]

    def beside(ref, k):
        here = rows8(ref, k)
        up = ref[:, 8 * k - 1 : 8 * k + 7, :] if k > 0 else pltpu.roll(here, 1, 1)
        down = ref[:, 8 * k + 1 : 8 * k + 9, :] if k < n_tile - 1 else pltpu.roll(here, 7, 1)
        one, other = pltpu.roll(here, 1, 2), pltpu.roll(here, LANES - 1, 2)
        left = jnp.where(lane == 0, jnp.concatenate([one[per - 1 :], one[: per - 1]], axis=0), one)
        right = jnp.where(lane == LANES - 1, jnp.concatenate([other[1:], other[:1]], axis=0), other)
        return (up + down) + (left + right)

    nothing = jnp.zeros((8, LANES), F32)
    own_tiles = range(1, n_tile - 1)

    nu0 = nothing
    for k in range(n_tile):
        f = rows8(field, k)
        w = rows8(inv, k) * f
        w0[:, 8 * k : 8 * k + 8, :] = w
        if k in own_tiles:
            nu0 = nu0 + jnp.sum(w * f, axis=0)

    def apply(w_old, w_new):
        a, b = nothing, nothing
        for k in range(n_tile):
            q = rows8(field, k) - beside(w_old, k)
            w = rows8(inv, k) * q
            field[:, 8 * k : 8 * k + 8, :] = q
            w_new[:, 8 * k : 8 * k + 8, :] = w
            if k in own_tiles:
                a = a + jnp.sum(rows8(w_old, k) * q, axis=0)
                b = b + jnp.sum(w * q, axis=0)
        return a, b

    nu1, nu2 = apply(w0, w1)
    nu3, nu4 = apply(w1, w2)
    nu5 = nothing
    for k in own_tiles:
        nu5 = nu5 + jnp.sum(rows8(w2, k) * (rows8(field, k) - beside(w2, k)), axis=0)

    gram_send[...] = jnp.zeros((8, LANES), F32)
    for k, nu in enumerate((nu0, nu1, nu2, nu3, nu4, nu5)):
        gram_send[k : k + 1, :] = jnp.sum(nu, axis=0, keepdims=True)
    gram_slot = pl.ds(pl.multiple_of(tile * 8, 8), 8)
    gram_recv[gram_slot, :] = gram_send[...]

    def gram_copy(target):
        return pltpu.make_async_remote_copy(
            src_ref=gram_send,
            dst_ref=gram_recv.at[gram_slot],
            send_sem=gram_ssem,
            recv_sem=gram_rsem,
            device_id=target,
            device_id_type=MESH,
        )

    for d in tile_offsets:
        gram_copy(tile_peer(d)).start()
    requests.wait_recv()
    asked = jnp.concatenate([req_v[8 * t : 8 * t + 1, :] for t in range(tiles)], axis=0)
    asked = jnp.concatenate([asked - tile * n_ocean, jnp.zeros((LANES - tiles, LANES), I32)], axis=0)
    asked = jnp.transpose(asked)
    where_col = lax.broadcasted_iota(I32, (nrows, n_ocean), 1)
    stacked = lax.rem(where_col, own) * per + lax.div(where_col, own)
    for t in range(tiles):
        hit = asked[0:nrows, t : t + 1] == stacked
        picks[t * nrows : (t + 1) * nrows, :] = jnp.where(hit, 1.0, 0.0).astype(BF16)

    gram_all = many(gram_recv, (tiles - 1) * 8, gram_ssem, gram_rsem)
    gram_all.wait_recv()
    total = jnp.sum(gram_recv[...].reshape(tiles, 8, LANES), axis=0)
    total = jnp.sum(total, axis=1, keepdims=True)
    n0, n1, n2, n3, n4, n5 = (total[k : k + 1, :] for k in range(6))

    def inverse(pivot, scale):
        good = pivot > 1e-6 * scale
        return jnp.where(good, 1.0 / jnp.where(good, pivot, 1.0), 0.0)

    i0 = inverse(n1, 0.0 * n1)
    l1, l2 = n2 * i0, n3 * i0
    d1, h = n3 - l1 * n2, n4 - l1 * n3
    i1 = inverse(d1, n3)
    l3 = h * i1
    d2 = n5 - l2 * n3 - l3 * h
    i2 = inverse(d2, n5)
    y1 = n1 - l1 * n0
    y2 = n2 - l2 * n0 - l3 * y1
    c2 = y2 * i2
    c1 = y1 * i1 - l3 * c2
    c0 = n0 * i0 - l1 * c1 - l2 * c2
    c0, c1, c2 = (jnp.broadcast_to(c, (1, LANES)) for c in (c0, c1, c2))

    loads["temp"].wait()
    for j in range(per):
        part = slice(j * LANES, (j + 1) * LANES)
        x = c0 * w0[j, HALO : HALO + own, :] + c1 * w1[j, HALO : HALO + own, :] + c2 * w2[j, HALO : HALO + own, :]
        height[:, part] = x
        sst[j * own : (j + 1) * own, :] = jnp.where(mask_ref[:, part] == 1, temp_ref[:, part] + x, 0.0).astype(BF16)

    rows_slot = pl.ds(pl.multiple_of(tile * nrows, nrows), nrows)
    wide_tiles = tiles // wide
    plane = lax.div(tile, wide_tiles)

    def rows_copy(other):
        return pltpu.make_async_remote_copy(
            src_ref=rows_send.at[pl.ds(pl.multiple_of(other * nrows, nrows), nrows)],
            dst_ref=rows_recv.at[rows_slot],
            send_sem=rows_ssem,
            recv_sem=rows_rsem,
            device_id=(group, other),
            device_id_type=MESH,
        )

    within = lax.rem(tile, wide_tiles)
    for dp in far_first(wide):
        goal = around(plane + dp, wide) * wide_tiles
        part = pl.ds(pl.multiple_of(goal * nrows, wide_tiles * nrows), wide_tiles * nrows)
        rows_send[part, :] = jnp.dot(picks[part, :], sst[...], preferred_element_type=F32).astype(BF16)
        for dt in far_first(wide_tiles):
            if dp or dt:
                rows_copy(goal + around(within + dt, wide_tiles)).start()
    rows_recv[rows_slot, :] = rows_send[rows_slot, :]
    rows_all = many(rows_recv, (tiles - 1) * nrows, rows_ssem, rows_rsem)
    rows_all.wait_recv()
    got = jnp.sum(rows_recv[...].astype(F32).reshape(tiles, nrows, LANES), axis=0)
    for k in range(nrows):
        rows_out[:, k * LANES : (k + 1) * LANES] = got[k : k + 1, :]

    requests.wait_send()
    many(flux_all, (n_chip - 1) * nrows, flux_ssem, flux_rsem.at[0]).wait_send()
    for g in range(groups):
        forward(g).wait_send()
    gram_all.wait_send()
    rows_all.wait_send()


def finish(pre, height, rows, column, atm_hbm, height_hbm, held, sems, height_sem):
    copy = pltpu.make_async_copy(height, height_hbm, height_sem)
    copy.start()
    lev, cols = pre.shape
    n_part = sems.shape[0]
    size = cols // n_part
    outs = []
    for i in range(n_part):
        part = pl.ds(i * size, size)
        for j in range(i * size, (i + 1) * size, LANES):
            held[:, j : j + LANES] = pre[:, j : j + LANES] + column[...] * rows[:, j : j + LANES]
        outs.append(pltpu.make_async_copy(held.at[:, part], atm_hbm.at[:, part], sems.at[i]))
        outs[-1].start()
    for out in outs:
        out.wait()
    copy.wait()


def solution(mesh):
    groups, tiles = mesh.shape["comp"], mesh.shape["tile"]
    count = groups * tiles

    def body(state, vco, weight, response, blocks, source, entry, present, mask, depth, temp, wanted):
        lev, cols = state.shape
        own, width = mask.shape
        nrows = cols // LANES
        n_flux = count * nrows
        n_ocean = own * width // LANES
        ext = own + 2 * HALO
        n_req = tiles * nrows
        n_chunk = max(1, cols // 1024)
        vmem = pl.BlockSpec(memory_space=pltpu.VMEM)
        n_block, n_entry = blocks.shape[0], source.shape[1]
        anywhere = pl.BlockSpec(memory_space=pltpu.HBM)
        dma = pltpu.SemaphoreType.DMA
        pre, height, rows, column = pl.pallas_call(
            functools.partial(kernel, groups, tiles),
            out_shape=(
                jax.ShapeDtypeStruct((lev, cols), F32),
                jax.ShapeDtypeStruct((own, width), F32),
                jax.ShapeDtypeStruct((1, cols), F32),
                jax.ShapeDtypeStruct((lev, LANES), F32),
            ),
            in_specs=[anywhere] * 12,
            out_specs=(vmem, vmem, vmem, vmem),
            scratch_shapes=[
                pltpu.VMEM((lev, cols), F32),
                pltpu.VMEM((lev, lev), F32),
                pltpu.VMEM((1, lev), F32),
                pltpu.VMEM((n_block, LANES, LANES), BF16),
                pltpu.VMEM((n_entry, n_ocean), I32),
                pltpu.VMEM((n_entry, n_ocean), I32),
                pltpu.VMEM((n_entry, n_ocean), I32),
                pltpu.VMEM((own, width), I32),
                pltpu.VMEM((own, width), F32),
                pltpu.VMEM((own, width), F32),
                pltpu.VMEM((1, nrows), I32),
                pltpu.VMEM((1, lev), F32),
                pltpu.VMEM((2 * lev, 2 * lev), BF16),
                pltpu.VMEM((nrows, LANES), F32),
                pltpu.VMEM((n_flux, LANES), BF16),
                pltpu.VMEM((n_block * n_flux + 8, LANES), F32),
                pltpu.VMEM((n_entry, 1, n_ocean + 2 * LANES), I32),
                pltpu.SMEM(((n_entry + 1) * (n_ocean + 2 * LANES),), I32),
                pltpu.VMEM((ext, width), F32),
                pltpu.VMEM((width // LANES, ext, LANES), F32),
                pltpu.VMEM((width // LANES, ext, LANES), F32),
                pltpu.VMEM((width // LANES, ext, LANES), F32),
                pltpu.VMEM((width // LANES, ext, LANES), F32),
                pltpu.VMEM((width // LANES, ext, LANES), F32),
                pltpu.VMEM((tiles * 8, LANES), I32),
                pltpu.VMEM((n_req, n_ocean), BF16),
                pltpu.VMEM((n_ocean, LANES), BF16),
                pltpu.VMEM((n_req, LANES), BF16),
                pltpu.VMEM((n_req, LANES), BF16),
                pltpu.VMEM((8, LANES), F32),
                pltpu.VMEM((tiles * 8, LANES), F32),
                dma((n_chunk,)),
                dma((11,)),
                dma((n_entry,)),
                dma,
                dma((groups,)),
                dma((groups,)),
                dma((groups,)),
                dma,
                dma,
                dma((4,)),
                dma((4,)),
                dma,
                dma,
                dma,
                dma,
            ],
            compiler_params=pltpu.CompilerParams(
                collective_id=0, has_side_effects=True, vmem_limit_bytes=48 * 1024 * 1024
            ),
        )(
            *(
                pltpu.with_memory_space_constraint(value, pltpu.HBM)
                for value in (
                    state,
                    vco,
                    weight[None, :],
                    blocks,
                    source.T,
                    entry.T,
                    present.T,
                    mask,
                    depth,
                    temp,
                    wanted[None, :],
                    response[None, :],
                )
            )
        )
        return pl.pallas_call(
            finish,
            out_shape=(jax.ShapeDtypeStruct((lev, cols), F32), jax.ShapeDtypeStruct((own, width), F32)),
            in_specs=[vmem] * 4,
            out_specs=(anywhere, anywhere),
            scratch_shapes=[pltpu.VMEM((lev, cols), F32), dma((n_chunk,)), dma],
            compiler_params=pltpu.CompilerParams(vmem_limit_bytes=16 * 1024 * 1024),
        )(pre, height, rows, column)

    split = P(None, ("comp", "tile"))
    ocean = P("tile", None)
    return jax.shard_map(
        body,
        mesh=mesh,
        in_specs=(split, P(), P(), P(), P(), ocean, ocean, ocean, ocean, ocean, ocean, P(("comp", "tile"))),
        out_specs=(split, ocean),
        check_vma=False,
    )
```

```python
import functools

import jax
import jax.numpy as jnp
from jax import lax
from jax.experimental import pallas as pl
from jax.experimental.pallas import tpu as pltpu
from jax.sharding import PartitionSpec as P

F32, BF16, I32 = jnp.float32, jnp.bfloat16, jnp.int32
MESH = pl.DeviceIdType.MESH
LANES = 128
HALO = 8
TIME_STEP = 0.5


FAR_FIRST = True


def hops(i, n):
    return min(i, n - i)


def kernel(
    groups,
    tiles,
    state_hbm,
    vco_hbm,
    weight_hbm,
    blocks_hbm,
    source_hbm,
    entry_hbm,
    present_hbm,
    mask_hbm,
    depth_hbm,
    temp_hbm,
    wanted_hbm,
    response_hbm,
    pre,
    height,
    rows_out,
    column_out,
    state,
    vco_ref,
    weight_ref,
    blocks_ref,
    source_ref,
    entry_ref,
    present_ref,
    mask_ref,
    depth_ref,
    temp_ref,
    wanted_ref,
    response_ref,
    vv,
    fluxf,
    flux_all,
    table,
    idx_v,
    idx_s,
    coef,
    inv,
    field,
    w0,
    w1,
    w2,
    req_v,
    picks,
    sst,
    rows_send,
    rows_recv,
    gram_send,
    gram_recv,
    in_sem,
    load_sem,
    idx_sem,
    flux_ssem,
    flux_rsem,
    fwd_ssem,
    fwd_rsem,
    req_ssem,
    req_rsem,
    halo_ssem,
    halo_rsem,
    gram_ssem,
    gram_rsem,
    rows_ssem,
    rows_rsem,
):
    group, tile = lax.axis_index("comp"), lax.axis_index("tile")
    count = groups * tiles
    lev, cols = state.shape
    own, width = mask_hbm.shape
    per = width // LANES
    ext = own + 2 * HALO
    nrows = cols // LANES
    n_flux = count * nrows
    n_entry, n_ocean = source_hbm.shape
    n_block = blocks_ref.shape[0]
    chunk = min(1024, cols)
    n_chunk = cols // chunk
    core, side = lax.rem(tile, 2), tiles // 2
    n_chip = groups * side
    partner = tile + 1 - 2 * core
    half = n_flux // 2
    part_rows = side * nrows
    span = n_ocean + 2 * LANES

    lane_of_chip = lax.div(tile, 2)
    chip = group * side + lane_of_chip

    def around(value, size):
        return jnp.where(value >= size, value - size, value)

    def far_first(n):
        return sorted(range(n), key=lambda i: -min(i, n - i))

    wide = 4 if side % 4 == 0 else 1
    chip_order = [a * (side // wide) + b for a in far_first(wide) for b in far_first(side // wide)]
    chip_order.sort(key=lambda q: -(hops(q // (side // wide), wide) + hops(q % (side // wide), side // wide)))
    order = far_first(groups) if FAR_FIRST else far_first(groups)[::-1]

    def chip_peer(dg, dq):
        return around(group + dg, groups), 2 * around(lane_of_chip + dq, side) + core

    def tile_peer(dt):
        return group, around(tile + dt, tiles)

    chip_offsets = [(dg, dq) for dg in order for dq in chip_order if dg or dq]
    across = side // wide

    def distance(offset):
        dg, dq = offset
        return hops(dg, groups) + hops(dq // across, wide) + hops(dq % across, across)

    chip_offsets.sort(key=lambda offset: -distance(offset))
    tile_offsets = [2 * dq + dc for dq in chip_order for dc in (0, 1) if dq or dc]

    loads = {
        name: pltpu.make_async_copy(source, target, load_sem.at[i])
        for i, (name, source, target) in enumerate(
            (
                ("vco", vco_hbm, vco_ref),
                ("weight", weight_hbm, weight_ref),
                ("mask", mask_hbm, mask_ref),
                ("depth", depth_hbm, depth_ref),
                ("source", source_hbm, source_ref),
                ("entry", entry_hbm, entry_ref),
                ("present", present_hbm, present_ref),
                ("wanted", wanted_hbm, wanted_ref),
                ("blocks", blocks_hbm, blocks_ref),
                ("temp", temp_hbm, temp_ref),
                ("response", response_hbm, response_ref),
            )
        )
    }

    def load_state(i):
        part = pl.ds(i * chunk, chunk)
        return pltpu.make_async_copy(state_hbm.at[:, part], state.at[:, part], in_sem)

    barrier = pltpu.get_barrier_semaphore()
    greeted = [chip_peer(*d) for d in chip_offsets]
    greeted += [(group, 2 * around(lane_of_chip + dq, side) + 1 - core) for dq in chip_order]

    def greet(targets):
        for target in targets:
            pl.semaphore_signal(barrier, inc=1, device_id=target, device_id_type=MESH)

    greet(greeted[:8])
    loads["vco"].start()
    for i in range(n_chunk):
        load_state(i).start()
    greet(greeted[8:])
    loads["weight"].start()
    for name in loads:
        if name not in ("vco", "weight"):
            loads[name].start()

    loads["vco"].wait()
    vco = vco_ref[...]
    v_hi = vco.astype(BF16)
    v_lo = (vco - v_hi.astype(F32)).astype(BF16)
    vv[0:lev, 0:lev] = v_hi
    vv[0:lev, lev : 2 * lev] = v_hi
    vv[lev : 2 * lev, 0:lev] = v_lo
    vv[lev : 2 * lev, lev : 2 * lev] = v_lo

    def tendency(s):
        hi = s.astype(BF16)
        lo = (s - hi.astype(F32)).astype(BF16)
        both = jnp.dot(vv[...], jnp.concatenate([hi, lo], axis=0), preferred_element_type=F32)
        return TIME_STEP * jnp.tanh(both[0:lev] + both[lev : 2 * lev])

    pltpu.make_async_copy(state_hbm, state, in_sem).wait()
    loads["weight"].wait()
    column = jnp.transpose(jnp.broadcast_to(weight_ref[...], (LANES, lev)))[:, 0:1]
    parts = [pl.ds(i * chunk, chunk) for i in range(n_chunk)]
    for part in parts:
        s = state[:, part]
        state[:, part] = s + tendency(s)
    for i, part in enumerate(parts):
        s = state[:, part]
        s = s + tendency(s)
        state[:, part] = s
        line = jnp.sum(s * column, axis=0, keepdims=True)
        for k in range(chunk // LANES):
            fluxf[i * (chunk // LANES) + k : i * (chunk // LANES) + k + 1, :] = line[:, k * LANES : (k + 1) * LANES]
    mine = pl.ds(pl.multiple_of(core * half + chip * nrows, nrows), nrows)
    flux_all[mine, :] = fluxf[...].astype(BF16)

    for name in ("source", "entry", "present"):
        loads[name].wait()
    spare = n_block * n_flux
    source = source_ref[...]
    holder = lax.div(source, nrows)
    row = lax.rem(holder, 2) * half + lax.div(holder, 2) * nrows + lax.rem(source, nrows)
    index = jnp.where(present_ref[...] == 1, entry_ref[...] * n_flux + row, jnp.full(source.shape, spare, I32))
    for k in range(n_entry):
        idx_v[k, :, LANES : LANES + n_ocean] = index[k : k + 1, :]
    table[pl.ds(spare, 8), :] = jnp.zeros((8, LANES), F32)

    pl.semaphore_wait(barrier, n_chip - 1 + side)

    def many(ref, rows, send_sem, recv_sem):
        return pltpu.make_async_remote_copy(
            src_ref=ref.at[pl.ds(0, rows)],
            dst_ref=ref.at[pl.ds(0, rows)],
            send_sem=send_sem,
            recv_sem=recv_sem,
            device_id=(group, partner),
            device_id_type=MESH,
        )

    after, before = lax.rem(tile + 1, tiles), lax.rem(tile + tiles - 1, tiles)

    def halo(ref, src, dst, k, target):
        return pltpu.make_async_remote_copy(
            src_ref=ref.at[src],
            dst_ref=ref.at[dst],
            send_sem=halo_ssem.at[k],
            recv_sem=halo_rsem.at[k],
            device_id=(group, target),
            device_id_type=MESH,
        )

    everything = slice(None)
    halos = (
        halo(coef, (pl.ds(own, HALO), everything), (pl.ds(0, HALO), everything), 0, after),
        halo(coef, (pl.ds(HALO, HALO), everything), (pl.ds(HALO + own, HALO), everything), 1, before),
        halo(idx_v, (everything, everything, pl.ds(n_ocean, LANES)), (everything, everything, pl.ds(0, LANES)), 2, after),
        halo(
            idx_v,
            (everything, everything, pl.ds(LANES, LANES)),
            (everything, everything, pl.ds(LANES + n_ocean, LANES)),
            3,
            before,
        ),
    )
    for copy in halos[2:]:
        copy.start()

    def flux_copy(target):
        return pltpu.make_async_remote_copy(
            src_ref=flux_all.at[mine],
            dst_ref=flux_all.at[mine],
            send_sem=flux_ssem,
            recv_sem=flux_rsem.at[group],
            device_id=target,
            device_id_type=MESH,
        )

    for d in chip_offsets:
        flux_copy(chip_peer(*d)).start()

    for name in ("mask", "depth", "wanted"):
        loads[name].wait()
    coef[HALO : HALO + own, :] = mask_ref[...].astype(F32) * (4.0 + depth_ref[...])
    own_slot = pl.ds(pl.multiple_of(tile * 8, 8), 8)
    req_v[own_slot, :] = jnp.full((8, LANES), -1, I32)
    req_v[own_slot, 0:nrows] = jnp.broadcast_to(wanted_ref[...], (8, nrows))

    def request(target):
        return pltpu.make_async_remote_copy(
            src_ref=req_v.at[own_slot],
            dst_ref=req_v.at[own_slot],
            send_sem=req_ssem,
            recv_sem=req_rsem,
            device_id=target,
            device_id_type=MESH,
        )

    for d in tile_offsets:
        request(tile_peer(d)).start()
    requests = many(req_v, (tiles - 1) * 8, req_ssem, req_rsem)

    for copy in halos[:2]:
        copy.start()

    for i in range(n_chunk):
        part = pl.ds(i * chunk, chunk)
        s = state[:, part]
        pre[:, part] = s + tendency(s)

    loads["response"].wait()
    column_out[...] = TIME_STEP * jnp.transpose(jnp.broadcast_to(response_ref[...], (LANES, lev)))

    zero_rows = jnp.zeros((per, HALO, LANES), F32)
    field[:, 0:HALO, :] = zero_rows
    field[:, HALO + own : ext, :] = zero_rows

    def reciprocal(value):
        return jnp.where(value > 0.0, 1.0 / jnp.where(value > 0.0, value, 1.0), 0.0)

    def set_inverse(first, last, exists):
        for j in range(per):
            value = reciprocal(coef[first:last, j * LANES : (j + 1) * LANES])
            inv[j, first:last, :] = value if exists is None else jnp.where(exists, value, 0.0)

    set_inverse(HALO, HALO + own, None)

    loads["blocks"].wait()
    pairs = [jnp.concatenate([blocks_ref[b], blocks_ref[b + 1]], axis=1) for b in range(0, n_block, 2)]

    def products(at):
        some = flux_all[pl.ds(pl.multiple_of(at, part_rows), part_rows), :]
        for b, pair in enumerate(pairs):
            got = jnp.dot(some, pair, preferred_element_type=F32)
            for k in range(2):
                to = pl.multiple_of((2 * b + k) * n_flux + at, part_rows)
                table[pl.ds(to, part_rows), :] = got[:, k * LANES : (k + 1) * LANES]

    def forward(g):
        slot = pl.ds(pl.multiple_of(core * half + g * part_rows, part_rows), part_rows)
        return pltpu.make_async_remote_copy(
            src_ref=flux_all.at[slot],
            dst_ref=flux_all.at[slot],
            send_sem=fwd_ssem,
            recv_sem=fwd_rsem.at[g],
            device_id=(group, partner),
            device_id_type=MESH,
        )

    def take(offset):
        g = around(group + offset, groups)
        blocks_in = side - 1 if offset == 0 else side
        many(flux_all, blocks_in * nrows, flux_ssem, flux_rsem.at[g]).wait_recv()
        forward(g).start()

    def near(offset):
        products(core * half + around(group + offset, groups) * part_rows)

    def far(offset):
        products((1 - core) * half + around(group + offset, groups) * part_rows)

    def shared(offset):
        forward(around(group + offset, groups)).wait_recv()

    ahead, behind = order[: len(order) // 2], order[len(order) // 2 :]

    @pl.when(core == 1)
    def _():
        for offset in ahead:
            take(offset)
            near(offset)
        for offset in behind:
            take(offset)
        for offset in behind:
            near(offset)

    @pl.when(core == 0)
    def _():
        for offset in ahead:
            shared(offset)
            far(offset)
        for offset in ahead:
            take(offset)
        for offset in ahead:
            near(offset)
        for offset in behind:
            take(offset)

    for copy in halos[2:]:
        copy.wait()
    index_copies = [
        pltpu.make_async_copy(idx_v.at[k, 0], idx_s.at[pl.ds(k * span, span)], idx_sem.at[k]) for k in range(n_entry)
    ]
    for copy in index_copies:
        copy.start()

    @pl.when(core == 1)
    def _():
        for some in (ahead, behind):
            for offset in some:
                shared(offset)
            for offset in some:
                far(offset)

    @pl.when(core == 0)
    def _():
        for offset in behind:
            shared(offset)
        for offset in behind:
            far(offset)
            near(offset)

    def forcing_rows(g_tile, j, rows):
        first_row = g_tile * 8 * per + j + (rows[0] - HALO) * per + LANES
        totals = []
        for s in rows:
            e = first_row + (s - rows[0]) * per
            got = [table[pl.ds(idx_s.at[pl.ds(e + k * span, 1)][0], 1), :] for k in range(n_entry)]
            while len(got) > 1:
                got = [sum(got[k : k + 2][1:], got[k]) for k in range(0, len(got), 2)]
            totals.append(got[0])
        at = pl.multiple_of(g_tile * 8, 8)
        block = field.at[j, pl.ds(at, 8), :]
        for s, total in zip(rows, totals):
            block[s : s + 1, :] = total

    def edge(j, carry):
        forcing_rows(0, j, (HALO - 3, HALO - 2, HALO - 1))
        forcing_rows(ext // 8 - 1, j, (0, 1, 2))
        return carry

    for copy in index_copies:
        copy.wait()
    lax.fori_loop(0, per, edge, 0)

    def inside_rows(g_tile, carry):
        def one(j, inner):
            forcing_rows(g_tile, j, range(8))
            return inner

        return lax.fori_loop(0, per, one, carry, unroll=5)

    lax.fori_loop(1, 1 + own // 8, inside_rows, 0)

    for copy in halos[:2]:
        copy.wait()
    set_inverse(0, HALO, tile > 0)
    set_inverse(HALO + own, ext, tile < tiles - 1)

    n_tile = ext // 8
    lane = lax.broadcasted_iota(I32, (per, 8, LANES), 2)

    def rows8(ref, k):
        return ref[:, 8 * k : 8 * k + 8, :]

    def beside(ref, k):
        here = rows8(ref, k)
        up = ref[:, 8 * k - 1 : 8 * k + 7, :] if k > 0 else pltpu.roll(here, 1, 1)
        down = ref[:, 8 * k + 1 : 8 * k + 9, :] if k < n_tile - 1 else pltpu.roll(here, 7, 1)
        one, other = pltpu.roll(here, 1, 2), pltpu.roll(here, LANES - 1, 2)
        left = jnp.where(lane == 0, jnp.concatenate([one[per - 1 :], one[: per - 1]], axis=0), one)
        right = jnp.where(lane == LANES - 1, jnp.concatenate([other[1:], other[:1]], axis=0), other)
        return (up + down) + (left + right)

    nothing = jnp.zeros((8, LANES), F32)
    own_tiles = range(1, n_tile - 1)

    nu0 = nothing
    for k in range(n_tile):
        f = rows8(field, k)
        w = rows8(inv, k) * f
        w0[:, 8 * k : 8 * k + 8, :] = w
        if k in own_tiles:
            nu0 = nu0 + jnp.sum(w * f, axis=0)

    def apply(w_old, w_new):
        a, b = nothing, nothing
        for k in range(n_tile):
            q = rows8(field, k) - beside(w_old, k)
            w = rows8(inv, k) * q
            field[:, 8 * k : 8 * k + 8, :] = q
            w_new[:, 8 * k : 8 * k + 8, :] = w
            if k in own_tiles:
                a = a + jnp.sum(rows8(w_old, k) * q, axis=0)
                b = b + jnp.sum(w * q, axis=0)
        return a, b

    nu1, nu2 = apply(w0, w1)
    nu3, nu4 = apply(w1, w2)
    nu5 = nothing
    for k in own_tiles:
        nu5 = nu5 + jnp.sum(rows8(w2, k) * (rows8(field, k) - beside(w2, k)), axis=0)

    gram_send[...] = jnp.zeros((8, LANES), F32)
    for k, nu in enumerate((nu0, nu1, nu2, nu3, nu4, nu5)):
        gram_send[k : k + 1, :] = jnp.sum(nu, axis=0, keepdims=True)
    gram_slot = pl.ds(pl.multiple_of(tile * 8, 8), 8)
    gram_recv[gram_slot, :] = gram_send[...]

    def gram_copy(target):
        return pltpu.make_async_remote_copy(
            src_ref=gram_send,
            dst_ref=gram_recv.at[gram_slot],
            send_sem=gram_ssem,
            recv_sem=gram_rsem,
            device_id=target,
            device_id_type=MESH,
        )

    for d in tile_offsets:
        gram_copy(tile_peer(d)).start()
    requests.wait_recv()
    asked = jnp.concatenate([req_v[8 * t : 8 * t + 1, :] for t in range(tiles)], axis=0)
    asked = jnp.concatenate([asked - tile * n_ocean, jnp.zeros((LANES - tiles, LANES), I32)], axis=0)
    asked = jnp.transpose(asked)
    where_col = lax.broadcasted_iota(I32, (nrows, n_ocean), 1)
    stacked = lax.rem(where_col, own) * per + lax.div(where_col, own)
    for t in range(tiles):
        hit = asked[0:nrows, t : t + 1] == stacked
        picks[t * nrows : (t + 1) * nrows, :] = jnp.where(hit, 1.0, 0.0).astype(BF16)

    gram_all = many(gram_recv, (tiles - 1) * 8, gram_ssem, gram_rsem)
    gram_all.wait_recv()
    total = jnp.sum(gram_recv[...].reshape(tiles, 8, LANES), axis=0)
    total = jnp.sum(total, axis=1, keepdims=True)
    n0, n1, n2, n3, n4, n5 = (total[k : k + 1, :] for k in range(6))

    def inverse(pivot, scale):
        good = pivot > 1e-6 * scale
        return jnp.where(good, 1.0 / jnp.where(good, pivot, 1.0), 0.0)

    i0 = inverse(n1, 0.0 * n1)
    l1, l2 = n2 * i0, n3 * i0
    d1, h = n3 - l1 * n2, n4 - l1 * n3
    i1 = inverse(d1, n3)
    l3 = h * i1
    d2 = n5 - l2 * n3 - l3 * h
    i2 = inverse(d2, n5)
    y1 = n1 - l1 * n0
    y2 = n2 - l2 * n0 - l3 * y1
    c2 = y2 * i2
    c1 = y1 * i1 - l3 * c2
    c0 = n0 * i0 - l1 * c1 - l2 * c2
    c0, c1, c2 = (jnp.broadcast_to(c, (1, LANES)) for c in (c0, c1, c2))

    loads["temp"].wait()
    for j in range(per):
        part = slice(j * LANES, (j + 1) * LANES)
        x = c0 * w0[j, HALO : HALO + own, :] + c1 * w1[j, HALO : HALO + own, :] + c2 * w2[j, HALO : HALO + own, :]
        height[:, part] = x
        sst[j * own : (j + 1) * own, :] = jnp.where(mask_ref[:, part] == 1, temp_ref[:, part] + x, 0.0).astype(BF16)

    rows_slot = pl.ds(pl.multiple_of(tile * nrows, nrows), nrows)
    wide_tiles = tiles // wide
    plane = lax.div(tile, wide_tiles)

    def rows_copy(other):
        return pltpu.make_async_remote_copy(
            src_ref=rows_send.at[pl.ds(pl.multiple_of(other * nrows, nrows), nrows)],
            dst_ref=rows_recv.at[rows_slot],
            send_sem=rows_ssem,
            recv_sem=rows_rsem,
            device_id=(group, other),
            device_id_type=MESH,
        )

    within = lax.rem(tile, wide_tiles)
    for dp in far_first(wide):
        goal = around(plane + dp, wide) * wide_tiles
        part = pl.ds(pl.multiple_of(goal * nrows, wide_tiles * nrows), wide_tiles * nrows)
        rows_send[part, :] = jnp.dot(picks[part, :], sst[...], preferred_element_type=F32).astype(BF16)
        for dt in far_first(wide_tiles):
            if dp or dt:
                rows_copy(goal + around(within + dt, wide_tiles)).start()
    rows_recv[rows_slot, :] = rows_send[rows_slot, :]
    rows_all = many(rows_recv, (tiles - 1) * nrows, rows_ssem, rows_rsem)
    rows_all.wait_recv()
    got = jnp.sum(rows_recv[...].astype(F32).reshape(tiles, nrows, LANES), axis=0)
    for k in range(nrows):
        rows_out[:, k * LANES : (k + 1) * LANES] = got[k : k + 1, :]

    requests.wait_send()
    many(flux_all, (n_chip - 1) * nrows, flux_ssem, flux_rsem.at[0]).wait_send()
    many(flux_all, half, fwd_ssem, flux_rsem.at[0]).wait_send()
    gram_all.wait_send()
    rows_all.wait_send()


def finish(pre, height, rows, column, atm_hbm, height_hbm, held, sems, height_sem):
    copy = pltpu.make_async_copy(height, height_hbm, height_sem)
    copy.start()
    lev, cols = pre.shape
    n_part = sems.shape[0]
    size = cols // n_part
    outs = []
    for i in range(n_part):
        part = pl.ds(i * size, size)
        for j in range(i * size, (i + 1) * size, LANES):
            held[:, j : j + LANES] = pre[:, j : j + LANES] + column[...] * rows[:, j : j + LANES]
        outs.append(pltpu.make_async_copy(held.at[:, part], atm_hbm.at[:, part], sems.at[i]))
        outs[-1].start()
    for out in outs:
        out.wait()
    copy.wait()


def solution(mesh):
    groups, tiles = mesh.shape["comp"], mesh.shape["tile"]
    count = groups * tiles

    def body(state, vco, weight, response, blocks, source, entry, present, mask, depth, temp, wanted):
        lev, cols = state.shape
        own, width = mask.shape
        nrows = cols // LANES
        n_flux = count * nrows
        n_ocean = own * width // LANES
        ext = own + 2 * HALO
        n_req = tiles * nrows
        n_chunk = max(1, cols // 1024)
        vmem = pl.BlockSpec(memory_space=pltpu.VMEM)
        n_block, n_entry = blocks.shape[0], source.shape[1]
        anywhere = pl.BlockSpec(memory_space=pltpu.HBM)
        dma = pltpu.SemaphoreType.DMA
        pre, height, rows, column = pl.pallas_call(
            functools.partial(kernel, groups, tiles),
            out_shape=(
                jax.ShapeDtypeStruct((lev, cols), F32),
                jax.ShapeDtypeStruct((own, width), F32),
                jax.ShapeDtypeStruct((1, cols), F32),
                jax.ShapeDtypeStruct((lev, LANES), F32),
            ),
            in_specs=[anywhere] * 12,
            out_specs=(vmem, vmem, vmem, vmem),
            scratch_shapes=[
                pltpu.VMEM((lev, cols), F32),
                pltpu.VMEM((lev, lev), F32),
                pltpu.VMEM((1, lev), F32),
                pltpu.VMEM((n_block, LANES, LANES), BF16),
                pltpu.VMEM((n_entry, n_ocean), I32),
                pltpu.VMEM((n_entry, n_ocean), I32),
                pltpu.VMEM((n_entry, n_ocean), I32),
                pltpu.VMEM((own, width), I32),
                pltpu.VMEM((own, width), F32),
                pltpu.VMEM((own, width), F32),
                pltpu.VMEM((1, nrows), I32),
                pltpu.VMEM((1, lev), F32),
                pltpu.VMEM((2 * lev, 2 * lev), BF16),
                pltpu.VMEM((nrows, LANES), F32),
                pltpu.VMEM((n_flux, LANES), BF16),
                pltpu.VMEM((n_block * n_flux + 8, LANES), F32),
                pltpu.VMEM((n_entry, 1, n_ocean + 2 * LANES), I32),
                pltpu.SMEM(((n_entry + 1) * (n_ocean + 2 * LANES),), I32),
                pltpu.VMEM((ext, width), F32),
                pltpu.VMEM((width // LANES, ext, LANES), F32),
                pltpu.VMEM((width // LANES, ext, LANES), F32),
                pltpu.VMEM((width // LANES, ext, LANES), F32),
                pltpu.VMEM((width // LANES, ext, LANES), F32),
                pltpu.VMEM((width // LANES, ext, LANES), F32),
                pltpu.VMEM((tiles * 8, LANES), I32),
                pltpu.VMEM((n_req, n_ocean), BF16),
                pltpu.VMEM((n_ocean, LANES), BF16),
                pltpu.VMEM((n_req, LANES), BF16),
                pltpu.VMEM((n_req, LANES), BF16),
                pltpu.VMEM((8, LANES), F32),
                pltpu.VMEM((tiles * 8, LANES), F32),
                dma,
                dma((11,)),
                dma((n_entry,)),
                dma,
                dma((groups,)),
                dma,
                dma((groups,)),
                dma,
                dma,
                dma((4,)),
                dma((4,)),
                dma,
                dma,
                dma,
                dma,
            ],
            compiler_params=pltpu.CompilerParams(
                collective_id=0, has_side_effects=True, vmem_limit_bytes=48 * 1024 * 1024
            ),
        )(
            *(
                pltpu.with_memory_space_constraint(value, pltpu.HBM)
                for value in (
                    state,
                    vco,
                    weight[None, :],
                    blocks,
                    source.T,
                    entry.T,
                    present.T,
                    mask,
                    depth,
                    temp,
                    wanted[None, :],
                    response[None, :],
                )
            )
        )
        return pl.pallas_call(
            finish,
            out_shape=(jax.ShapeDtypeStruct((lev, cols), F32), jax.ShapeDtypeStruct((own, width), F32)),
            in_specs=[vmem] * 4,
            out_specs=(anywhere, anywhere),
            scratch_shapes=[pltpu.VMEM((lev, cols), F32), dma((n_chunk,)), dma],
            compiler_params=pltpu.CompilerParams(vmem_limit_bytes=16 * 1024 * 1024),
        )(pre, height, rows, column)

    split = P(None, ("comp", "tile"))
    ocean = P("tile", None)
    return jax.shard_map(
        body,
        mesh=mesh,
        in_specs=(split, P(), P(), P(), P(), ocean, ocean, ocean, ocean, ocean, ocean, P(("comp", "tile"))),
        out_specs=(split, ocean),
        check_vma=False,
    )
```
